256 devices in a mesh: dp: 16 (over y, x), expert: 8 (over z), tensor: 2 (over core).
Axes of the slice: x: 4, y: 4, z: 8, core: 2. Of those that a mesh axis runs over, the one named last changes fastest.
Arguments:
- tokens: bfloat16 [2048, 4096], P(('dp', 'expert'), 'tensor'), may hold values from -6 to 6
- target: bfloat16 [2048, 4096], P(('dp', 'expert'), 'tensor'), may hold values from -4 to 4
- router: bfloat16 [4096, 8], P('tensor'), may hold values from -1 to 1
- w_gate: bfloat16 [8, 4096, 14336], P('expert', None, ('dp', 'tensor')), may hold values from -1 to 1
- w_up: bfloat16 [8, 4096, 14336], P('expert', None, ('dp', 'tensor')), may hold values from -1 to 1
- w_down: bfloat16 [8, 14336, 4096], P('expert', ('dp', 'tensor')), may hold values from -1 to 1
- expert_ids: int32 [2048, 2], P(('dp', 'expert')), may hold values from 0 to 7, as said below
- lengths: int32 [64], replicated, may hold values from 1 to 128, 2048 in all
- bench_ids: int32 [64], replicated, may hold values from 0 to 15
Outputs:
- mixed: bfloat16 [2048, 4096], P(('dp', 'expert'), 'tensor')
- bench_loss: float32 [16], replicated
- counts: int32 [16], replicated
The draws below stay inside these ranges and needn't reach their ends.
Inputs may be any that keep to these rules, and one draw needn't show every extreme that they name: `expert_ids`: each row names two different experts; among the 16 rows of one device no expert is named by more than 8 rows; for each index of dp, one expert is named by exactly 8 rows of every device of that index. The lengths sum to 2048.
All inputs are finite; a program needn't handle non-finite values.
Results may differ from the reference program's by a relative error of at most 0.0085.
Values may be sent and summed in bfloat16 or wider, within the bound.
A program may use at most 128 MiB of HBM per device.

```python
import math
import jax
import jax.numpy as jnp
import numpy as np
from jax import lax

D = 4096
FF = 14336
TOK_DEV = 16
NB = 16
EXPERTS = 8
CAP = 8
TOKENS = 2048
NSEQ = 64
SEQ_MOST = 128
N_DP = 16
N_EXPERT = 8


def normal_like(key, extent, spread):
    values = jax.random.normal(key, extent, jnp.float32) * spread
    return jnp.clip(values, -6.0 * spread, 6.0 * spread)


def token_draw(key):
    return normal_like(jax.random.fold_in(key, 101), (TOKENS, D), 1.0).astype(jnp.bfloat16)


def router_draw(key):
    return normal_like(jax.random.fold_in(key, 102), (D, EXPERTS), D ** (-0.5)).astype(jnp.bfloat16)


def expert_matrix(key, label, index, rows, columns):
    inner = jax.random.fold_in(jax.random.fold_in(key, label), index)
    return normal_like(inner, (rows, columns), rows ** (-0.5)).astype(jnp.bfloat16)


def expert_stack(key, label, rows, columns):
    return lax.map(lambda index: expert_matrix(key, label, index, rows, columns), jnp.arange(EXPERTS, dtype=jnp.int32))


def route_group(key, index):
    entries = EXPERTS * CAP
    kept_count = 2 * TOK_DEV
    common = jax.random.fold_in(jax.random.fold_in(key, 106), index // EXPERTS)
    own = jax.random.fold_in(jax.random.fold_in(key, 107), index)
    pick_key, order_key, flip_key = jax.random.split(own, 3)
    order = jax.random.permutation(common, EXPERTS).astype(jnp.int32)
    listing = jnp.repeat(order, CAP)
    position = jnp.arange(entries, dtype=jnp.int32)
    score = jax.random.randint(pick_key, (entries,), 0, 4096, dtype=jnp.int32) * entries + position
    score = jnp.where(position < CAP, position - entries, score).astype(jnp.int32)
    chosen = lax.top_k(-score, kept_count)[1]
    picks = listing[jnp.sort(chosen)]
    pairs = picks.reshape(2, TOK_DEV).T
    pairs = pairs[jax.random.permutation(order_key, TOK_DEV)]
    flip = jax.random.randint(flip_key, (TOK_DEV,), 0, 2, dtype=jnp.int32)
    front = jnp.where(flip == 1, pairs[:, 1], pairs[:, 0])
    back = jnp.where(flip == 1, pairs[:, 0], pairs[:, 1])
    return jnp.stack([front, back], axis=1).astype(jnp.int32)


def route_draw(key):
    groups = TOKENS // TOK_DEV
    blocks = lax.map(lambda index: route_group(key, index), jnp.arange(groups, dtype=jnp.int32))
    return blocks.reshape(TOKENS, 2).astype(jnp.int32)


def draw_tokens(key, part):
    return token_draw(key)


def draw_router(key, part):
    return router_draw(key)


def draw_w_gate(key, part):
    return expert_stack(key, 103, D, FF)


def draw_w_up(key, part):
    return expert_stack(key, 104, D, FF)


def draw_w_down(key, part):
    return expert_stack(key, 105, FF, D)


def draw_expert_ids(key, part):
    return route_draw(key)


def draw_target(key, part):
    tokens = token_draw(key).astype(jnp.float32)
    router = router_draw(key).astype(jnp.float32)
    expert_ids = route_draw(key)
    logits = jnp.dot(tokens, router, precision=lax.Precision.HIGHEST)
    chosen = expert_ids[:, :, None] == jnp.arange(EXPERTS, dtype=jnp.int32)[None, None, :]
    picked = jnp.sum(jnp.where(chosen, logits[:, None, :], jnp.float32(0.0)), axis=2)
    gates = jnp.stack([jax.nn.sigmoid(picked[:, 0] - picked[:, 1]), jax.nn.sigmoid(picked[:, 1] - picked[:, 0])], axis=1)
    half = TOKENS // 2
    counter = jnp.arange(TOKENS, dtype=jnp.int32)

    def add_expert(index, total):
        index = jnp.asarray(index).astype(jnp.int32)
        member = jnp.any(expert_ids == index, axis=1)
        rank = (jnp.where(member, 0, 1) * TOKENS + counter).astype(jnp.int32)
        rows_index = jnp.argsort(rank)[:half].astype(jnp.int32)
        weight = jnp.sum(jnp.where(expert_ids == index, gates, jnp.float32(0.0)), axis=1)[rows_index]
        rows = tokens[rows_index]
        gate_w = expert_matrix(key, 103, index, D, FF).astype(jnp.float32)
        up_w = expert_matrix(key, 104, index, D, FF).astype(jnp.float32)
        down_w = expert_matrix(key, 105, index, FF, D).astype(jnp.float32)
        gate = jnp.dot(rows, gate_w, precision=lax.Precision.HIGHEST)
        up = jnp.dot(rows, up_w, precision=lax.Precision.HIGHEST)
        hidden = jax.nn.silu(gate) * up
        output = jnp.dot(hidden, down_w, precision=lax.Precision.HIGHEST)
        return total.at[rows_index].add(weight[:, None] * output)
    mixed = lax.fori_loop(0, EXPERTS, add_expert, jnp.zeros((TOKENS, D), jnp.float32))
    rise = 1.0 + 2.0 * counter.astype(jnp.float32) / (TOKENS - 1)
    spread = 0.25 * rise
    noise = normal_like(jax.random.fold_in(key, 108), (TOKENS, D), spread[:, None])
    return jnp.clip(mixed + noise, -4.0, 4.0).astype(jnp.bfloat16)


def place_ends(values, key, least, largest):
    index_at = [jax.random.randint(jax.random.fold_in(key, axis), (), 0, length) for axis, length in enumerate(values.shape)]
    main_axis = values.shape.index(max(values.shape))
    neighbour = index_at[:main_axis] + [(index_at[main_axis] + 1) % values.shape[main_axis]] + index_at[main_axis + 1:]
    return values.at[tuple(index_at)].set(least).at[tuple(neighbour)].set(largest)


def profile(number_of, total, reach, skew):
    weights = [(1 << 20) // math.isqrt(grade ** skew) + 1 for grade in range(2, number_of + 1)]
    rest, given = total - reach - (number_of - 1), [1] * (number_of - 1)
    while rest > 0:
        free = [i for i in range(number_of - 1) if given[i] < reach]
        mass, budget = sum([weights[i] for i in free]), rest
        for i in free:
            extra = min(reach - given[i], max(1, budget * weights[i] // mass), rest)
            given[i] = given[i] + extra
            rest = rest - extra
    return np.array([reach] + given)


def uneven(key, count, total, most, lean):
    if count == 2:
        one = jax.random.randint(key, (), max(1, total - most), min(most, total - 1) + 1)
        return jnp.stack([one, total - one])
    sizes = jnp.asarray(profile(count, total, most, lean), jnp.int32)
    pairs = (count - 1) // 2
    source_of, receiver = sizes[1:1 + 2 * pairs:2], sizes[2:2 + 2 * pairs:2]
    slack = jnp.minimum(source_of - 1, most - receiver)
    passed = jax.random.randint(jax.random.fold_in(key, 1), (pairs,), 0, 1 << 20) % (slack + 1)
    sizes = sizes.at[1:1 + 2 * pairs:2].set(source_of - passed).at[2:2 + 2 * pairs:2].set(receiver + passed)
    return sizes[jax.random.permutation(jax.random.fold_in(key, 2), count)]


def setup_inputs(seed: int = 0) -> dict:
    keys = jax.random.split(jax.random.key(seed), 10)
    return {
        "tokens": draw_tokens(jax.random.fold_in(keys[9], 71), 0),
        "target": draw_target(jax.random.fold_in(keys[9], 71), 0),
        "router": draw_router(jax.random.fold_in(keys[9], 71), 0),
        "w_gate": draw_w_gate(jax.random.fold_in(keys[9], 71), 0),
        "w_up": draw_w_up(jax.random.fold_in(keys[9], 71), 0),
        "w_down": draw_w_down(jax.random.fold_in(keys[9], 71), 0),
        "expert_ids": draw_expert_ids(jax.random.fold_in(keys[9], 71), 0),
        "lengths": uneven(keys[7], NSEQ, TOKENS, SEQ_MOST, 2).astype(jnp.int32),
        "bench_ids": place_ends(jax.random.randint(keys[8], (NSEQ,), 0, NB), jax.random.fold_in(keys[8], 1), 0, NB - 1).astype(jnp.int32),
    }


def reference(tokens, target, router, w_gate, w_up, w_down, expert_ids, lengths, bench_ids):
    groups = N_DP * N_EXPERT
    logits = jnp.dot(tokens, router, preferred_element_type=jnp.float32)
    chosen = expert_ids[:, :, None] == jnp.arange(EXPERTS, dtype=jnp.int32)[None, None, :]
    picked = jnp.sum(jnp.where(chosen, logits[:, None, :], jnp.float32(0.0)), axis=2)
    first = jax.nn.sigmoid(picked[:, 0] - picked[:, 1])
    second = jax.nn.sigmoid(picked[:, 1] - picked[:, 0])
    marks = chosen.astype(jnp.int32).reshape(groups, TOK_DEV * 2, EXPERTS)
    before = jnp.cumsum(marks, axis=1) - marks
    slot = jnp.sum(before * marks, axis=2).reshape(TOKENS, 2).astype(jnp.int32)
    owner = (jnp.arange(TOKENS, dtype=jnp.int32) // TOK_DEV)[:, None] * jnp.ones((1, 2), jnp.int32)
    place = (owner * CAP + slot).astype(jnp.int32)
    token_index = jnp.arange(TOKENS, dtype=jnp.int32)[:, None] * jnp.ones((1, 2), jnp.int32)
    table = jnp.zeros((EXPERTS, groups * CAP), jnp.int32).at[expert_ids, place].set(token_index)
    filled = jnp.zeros((EXPERTS, groups * CAP), jnp.int32).at[expert_ids, place].set(1)

    def expert_rows(operands):
        gate_w, up_w, down_w, rows_index, live = operands
        rows = jnp.where(live[:, None] > 0, tokens[rows_index], jnp.zeros((), jnp.bfloat16))
        gate = jnp.dot(rows, gate_w, preferred_element_type=jnp.float32)
        up = jnp.dot(rows, up_w, preferred_element_type=jnp.float32)
        hidden = (jax.nn.silu(gate) * up).astype(jnp.bfloat16)
        return jnp.dot(hidden, down_w, preferred_element_type=jnp.float32).astype(jnp.bfloat16)

    outputs = lax.map(expert_rows, (w_gate, w_up, w_down, table, filled))
    y_first = outputs[expert_ids[:, 0], place[:, 0]].astype(jnp.float32)
    y_second = outputs[expert_ids[:, 1], place[:, 1]].astype(jnp.float32)
    mixed = (first[:, None] * y_first + second[:, None] * y_second).astype(jnp.bfloat16)

    ends = jnp.cumsum(lengths).astype(jnp.int32)
    starts = ends - lengths
    position = jnp.arange(TOKENS, dtype=jnp.int32)
    inside = ((position[:, None] >= starts[None, :]) & (position[:, None] < ends[None, :])).astype(jnp.float32)
    closing = jnp.any((position + 1)[:, None] == ends[None, :], axis=1)
    scored = jnp.where(closing, jnp.float32(0.0), jnp.float32(1.0))
    bench_table = (bench_ids[:, None] == jnp.arange(NB, dtype=jnp.int32)[None, :])
    bench_of = jnp.dot(inside, bench_table.astype(jnp.float32), precision=lax.Precision.HIGHEST)
    diff = mixed.astype(jnp.float32) - target.astype(jnp.float32)
    token_loss = jnp.sum(diff * diff, axis=1) / D
    loss_sum = jnp.dot(scored * token_loss, bench_of, precision=lax.Precision.HIGHEST)
    counts = jnp.sum(jnp.where(bench_table, (lengths - 1)[:, None], 0), axis=0).astype(jnp.int32)
    bench_loss = loss_sum / jnp.maximum(counts, 1).astype(jnp.float32)
    return mixed, bench_loss, counts
```

```python
import jax
import jax.numpy as jnp
from jax import lax
from jax.experimental import pallas as pl
from jax.experimental.pallas import tpu as pltpu
from jax.sharding import Mesh
from jax.sharding import PartitionSpec as P

D = 4096
DH = D // 2
NB = 16
CAP = 8
TOK = 16
HID = 448
NSEQ = 64
NE = 8
NQ = 2
FQ = DH // NQ
DP_EXPERT = ("dp_0", "dp_1", "expert")
DP_TENSOR = ("dp_0", "dp_1", "tensor")
MESH = pl.DeviceIdType.MESH
F32 = jnp.float32
BF16 = jnp.bfloat16
NSEMS = 62 * NQ + 40


def kernel(
    tokens, target, router, wg_hbm, wu_hbm, wd_hbm, ids, lengths, bench,
    mixed_out, loss_out, counts_out,
    OUT, ZL, XO, XP, WG, WU, WD, H, PX, PR, PO, S, R1, R2, TB, T1, T2, RET, BACK,
    LG, LGR, L1, L2, MIX, wsem, ssem, rsem,
):
    y = lax.axis_index("dp_0")
    x = lax.axis_index("dp_1")
    z = lax.axis_index("expert")
    c = lax.axis_index("tensor")

    def at(dy=0, dx=0, dz=0, dc=0):
        return {
            "dp_0": lax.rem(y + dy, 4),
            "dp_1": lax.rem(x + dx, 4),
            "expert": lax.rem(z + dz, 8),
            "tensor": lax.rem(c + dc, 2),
        }

    column = [(dz, dc) for dz in range(8) for dc in range(2)][1:]
    plane = [(dy, dx) for dy in range(4) for dx in range(4)][1:]
    barrier = pltpu.get_barrier_semaphore()
    for dz, dc in column:
        pl.semaphore_signal(barrier, inc=1, device_id=at(dz=dz, dc=dc), device_id_type=MESH)
    for dy, dx in plane:
        pl.semaphore_signal(barrier, inc=1, device_id=at(dy=dy, dx=dx), device_id_type=MESH)

    loads = []
    for half in range(2):
        first = pl.multiple_of(lax.rem(c + half, 2) * DH, DH)
        loads.append(pltpu.make_async_copy(wg_hbm.at[0, :, pl.ds(first, DH)], WG.at[half], wsem.at[3 * half]))
        loads.append(pltpu.make_async_copy(wu_hbm.at[0, :, pl.ds(first, DH)], WU.at[half], wsem.at[3 * half + 1]))
        loads.append(pltpu.make_async_copy(wd_hbm.at[0, :, pl.ds(first, DH)], WD.at[half], wsem.at[3 * half + 2]))
    for load in loads:
        load.start()

    started = []

    def send(src, dst, device):
        number = len(started)
        copy = pltpu.make_async_remote_copy(
            src_ref=src, dst_ref=dst, send_sem=ssem.at[number], recv_sem=rsem.at[number],
            device_id=device, device_id_type=MESH,
        )
        copy.start()
        started.append(copy)
        return copy

    lane = lax.broadcasted_iota(jnp.int32, (TOK, 128), 1)
    row16 = lax.broadcasted_iota(jnp.int32, (TOK, TOK), 0)
    col16 = lax.broadcasted_iota(jnp.int32, (TOK, TOK), 1)

    def as_column(row):
        spread = jnp.broadcast_to(row.astype(F32), (TOK, TOK))
        return jnp.sum(jnp.where(row16 == col16, spread, 0.0), axis=1, keepdims=True).astype(jnp.int32)

    id_0 = as_column(ids[0:1, :])
    id_1 = as_column(ids[1:2, :])
    marks_0 = jnp.where(lane == id_0, 1.0, 0.0)
    marks_1 = jnp.where(lane == id_1, 1.0, 0.0)
    earlier = jnp.where(col16 < row16, 1.0, 0.0).astype(BF16)
    before = jnp.dot(earlier, (marks_0 + marks_1).astype(BF16), preferred_element_type=F32)
    slot_0 = jnp.sum(before * marks_0, axis=1, keepdims=True)
    slot_1 = jnp.sum(before * marks_1, axis=1, keepdims=True)
    place_0 = (((id_0 - z + NE) & (NE - 1)) * CAP).astype(F32) + slot_0
    place_1 = (((id_1 - z + NE) & (NE - 1)) * CAP).astype(F32) + slot_1
    place = lax.broadcasted_iota(jnp.int32, (TOK, NE * CAP), 1).astype(F32)
    put_0 = jnp.where(place == place_0, 1.0, 0.0)
    put_1 = jnp.where(place == place_1, 1.0, 0.0)
    dispatch = (put_0 + put_1).astype(BF16)
    for q in range(NQ):
        lanes = pl.ds(q * FQ, FQ)
        rows = lax.dot_general(
            dispatch, tokens[:, lanes], (((0,), (0,)), ((), ())), preferred_element_type=F32
        )
        rows = rows.reshape(NE, CAP, FQ).astype(BF16)
        OUT[:, :, lanes] = rows
        ZL[0, :, lanes] = rows[0]
    by_rows = (((1,), (1,)), ((), ()))
    partial = lax.dot_general(tokens[...], router[...], by_rows, preferred_element_type=F32)
    LG[...] = jnp.zeros((TOK, 128), F32)
    LG[:, 0:NE] = partial

    pl.semaphore_wait(barrier, len(column) + len(plane))

    z_moves = []
    for q in range(NQ):
        lanes = pl.ds(q * FQ, FQ)
        z_moves.append(
            [send(OUT.at[j, :, lanes], ZL.at[8 - j, :, lanes], at(dz=j)) for j in (4, 3, 5, 2, 6, 1, 7)]
        )
    logits_move = send(LG, LGR, at(dc=1))

    def small_axis(ab, step):
        return at(dx=step) if ab == 0 else at(dy=step)

    def large_axis(ab, step):
        return at(dy=step) if ab == 0 else at(dx=step)

    near = []
    for q in range(NQ):
        lanes = pl.ds(q * FQ, FQ)
        for move in z_moves[q]:
            move.wait_recv()
        moves = []
        for ab in range(2):
            rows = ZL[4 * ab : 4 * ab + 4, :, lanes].astype(F32).reshape(32, FQ)
            XO[0, ab, 0:32, lanes] = rows.astype(BF16)
            src = XO.at[0, ab, 0:32, lanes]
            moves.append(send(src, XO.at[0, ab, 96:128, lanes], small_axis(ab, 1)))
            moves.append(send(src, XO.at[0, ab, 32:64, lanes], small_axis(ab, 3)))
        near.append(moves)
    far = []
    for q in range(NQ):
        lanes = pl.ds(q * FQ, FQ)
        moves = []
        for ab in range(2):
            near[q][2 * ab].wait_recv()
            moves.append(send(XO.at[0, ab, 96:112, lanes], XO.at[0, ab, 64:80, lanes], small_axis(ab, 1)))
            near[q][2 * ab + 1].wait_recv()
            moves.append(send(XO.at[0, ab, 48:64, lanes], XO.at[0, ab, 80:96, lanes], small_axis(ab, 3)))
        far.append(moves)
    near = []
    across = {}
    for q in range(NQ):
        lanes = pl.ds(q * FQ, FQ)
        moves = []
        for ab in range(2):
            far[q][2 * ab].wait_recv()
            far[q][2 * ab + 1].wait_recv()
            moves.append(send(XO.at[0, ab, :, lanes], XO.at[3, ab, :, lanes], large_axis(ab, 1)))
            moves.append(send(XO.at[0, ab, :, lanes], XO.at[1, ab, :, lanes], large_axis(ab, 3)))
        near.append(moves)
        across[0, q] = send(XO.at[0, :, :, lanes], XP.at[0, :, :, lanes], at(dc=1))

    for load in loads:
        load.wait()

    partner_sums = {}

    def compute(rel):
        own = XO[rel].reshape(256, DH)
        other = XP[rel].reshape(256, DH)
        gate = lax.dot_general(WG[0], own, by_rows, preferred_element_type=F32)
        gate += lax.dot_general(WG[1], other, by_rows, preferred_element_type=F32)
        up = lax.dot_general(WU[0], own, by_rows, preferred_element_type=F32)
        up += lax.dot_general(WU[1], other, by_rows, preferred_element_type=F32)
        H[...] = (gate * jax.nn.sigmoid(gate) * up).T.astype(BF16)

        def down_other(n, carry):
            cols = pl.ds(pl.multiple_of(n * 256, 256), 256)
            PX[rel, :, cols] = jnp.dot(H[...], WD[1, :, cols], preferred_element_type=F32).astype(BF16)
            return carry

        def down_own(n, carry):
            cols = pl.ds(pl.multiple_of(n * 256, 256), 256)
            PO[rel, :, cols] = jnp.dot(H[...], WD[0, :, cols], preferred_element_type=F32)
            return carry

        lax.fori_loop(0, DH // 256, down_other, 0)
        partner_sums[rel] = send(PX.at[rel], PR.at[rel], at(dc=1))
        lax.fori_loop(0, DH // 256, down_own, 0)

    for q in range(NQ):
        across[0, q].wait_recv()
    compute(0)

    far = []
    for q in range(NQ):
        lanes = pl.ds(q * FQ, FQ)
        moves = []
        for ab in range(2):
            near[q][2 * ab].wait_recv()
            moves.append(send(XO.at[3, ab, 0:64, lanes], XO.at[2, ab, 0:64, lanes], large_axis(ab, 1)))
            near[q][2 * ab + 1].wait_recv()
            moves.append(send(XO.at[1, ab, 64:128, lanes], XO.at[2, ab, 64:128, lanes], large_axis(ab, 3)))
        far.append(moves)
        for rel in (1, 3):
            across[rel, q] = send(XO.at[rel, :, :, lanes], XP.at[rel, :, :, lanes], at(dc=1))
    for rel in (1, 3):
        for q in range(NQ):
            across[rel, q].wait_recv()
        compute(rel)
    for q in range(NQ):
        lanes = pl.ds(q * FQ, FQ)
        for move in far[q]:
            move.wait_recv()
        across[2, q] = send(XO.at[2, :, :, lanes], XP.at[2, :, :, lanes], at(dc=1))

    direct = {}
    for rel in (1, 3):
        partner_sums[rel].wait_recv()
        S[rel] = (PO[rel] + PR[rel].astype(F32)).astype(BF16).reshape(2, 128, DH)
        for q in range(NQ):
            lanes = pl.ds(q * FQ, FQ)
            for ab in range(2):
                half = slice(64, 128) if rel == 1 else slice(0, 64)
                slot = 0 if rel == 1 else 1
                direct[rel, q, ab] = send(
                    S.at[rel, ab, half, lanes], R2.at[slot, ab, half, lanes], large_axis(ab, rel)
                )
    for q in range(NQ):
        across[2, q].wait_recv()
    compute(2)
    partner_sums[0].wait_recv()
    partner_sums[2].wait_recv()
    first = {}
    for q in range(NQ):
        lanes = pl.ds(q * FQ, FQ)
        S[2, :, :, lanes] = (PO[2, :, lanes] + PR[2, :, lanes].astype(F32)).astype(BF16).reshape(2, 128, FQ)
        for ab in range(2):
            first[q, ab, 1] = send(S.at[2, ab, 0:64, lanes], R1.at[ab, 0:64, lanes], large_axis(ab, 1))
            first[q, ab, 3] = send(S.at[2, ab, 64:128, lanes], R1.at[ab, 64:128, lanes], large_axis(ab, 3))
    second = {}
    for q in range(NQ):
        lanes = pl.ds(q * FQ, FQ)
        for ab in range(2):
            for rel, half, slot in ((1, slice(0, 64), 0), (3, slice(64, 128), 1)):
                first[q, ab, rel].wait_recv()
                S[rel, ab, half, lanes] = (
                    S[rel, ab, half, lanes].astype(F32) + R1[ab, half, lanes].astype(F32)
                ).astype(BF16)
                second[q, ab, rel] = send(
                    S.at[rel, ab, half, lanes], R2.at[slot, ab, half, lanes], large_axis(ab, rel)
                )
    direct_small = {}
    first_small = {}
    for q in range(NQ):
        lanes = pl.ds(q * FQ, FQ)
        for ab in range(2):
            block = slice(128 * ab, 128 * ab + 128)
            for rel in (1, 3):
                direct[rel, q, ab].wait_recv()
                second[q, ab, rel].wait_recv()
            total = PO[0, block, lanes] + PR[0, block, lanes].astype(F32)
            total += R2[0, ab, :, lanes].astype(F32)
            total += R2[1, ab, :, lanes].astype(F32)
            PO[0, block, lanes] = total
            TB[ab, :, lanes] = total.astype(BF16)
            first_small[q, ab, 1] = send(TB.at[ab, 64:80, lanes], T1.at[ab, 0:16, lanes], small_axis(ab, 1))
            first_small[q, ab, 3] = send(TB.at[ab, 80:96, lanes], T1.at[ab, 16:32, lanes], small_axis(ab, 3))
            direct_small[q, ab, 1] = send(TB.at[ab, 48:64, lanes], T2.at[0, ab, 16:32, lanes], small_axis(ab, 1))
            direct_small[q, ab, 3] = send(TB.at[ab, 96:112, lanes], T2.at[1, ab, 0:16, lanes], small_axis(ab, 3))
    second_small = {}
    for q in range(NQ):
        lanes = pl.ds(q * FQ, FQ)
        for ab in range(2):
            for rel, base, half, slot in ((1, 32, slice(0, 16), 0), (3, 96, slice(16, 32), 1)):
                first_small[q, ab, rel].wait_recv()
                mine = slice(base + half.start, base + half.stop)
                TB[ab, mine, lanes] = (
                    PO[0, 128 * ab + mine.start : 128 * ab + mine.stop, lanes] + T1[ab, half, lanes].astype(F32)
                ).astype(BF16)
                second_small[q, ab, rel] = send(
                    TB.at[ab, mine, lanes], T2.at[slot, ab, half, lanes], small_axis(ab, rel)
                )
    returns = []
    for q in range(NQ):
        lanes = pl.ds(q * FQ, FQ)
        for ab in range(2):
            for rel in (1, 3):
                direct_small[q, ab, rel].wait_recv()
                second_small[q, ab, rel].wait_recv()
            total = PO[0, 128 * ab : 128 * ab + 32, lanes]
            total += T2[0, ab, :, lanes].astype(F32)
            total += T2[1, ab, :, lanes].astype(F32)
            RET[4 * ab : 4 * ab + 4, :, lanes] = total.reshape(4, CAP, FQ).astype(BF16)
        BACK[0, :, lanes] = RET[0, :, lanes]
        returns.append(
            [send(RET.at[j, :, lanes], BACK.at[8 - j, :, lanes], at(dz=j)) for j in (4, 3, 5, 2, 6, 1, 7)]
        )

    logits_move.wait_recv()
    logits = LG[...] + LGR[...]
    picked_0 = jnp.sum(logits * marks_0, axis=1, keepdims=True)
    picked_1 = jnp.sum(logits * marks_1, axis=1, keepdims=True)
    gate_0 = jax.nn.sigmoid(picked_0 - picked_1)
    gate_1 = jax.nn.sigmoid(picked_1 - picked_0)
    weights = gate_0 * put_0 + gate_1 * put_1
    high = weights.astype(BF16)
    rest = weights - high.astype(F32)
    middle = rest.astype(BF16)
    low = (rest - middle.astype(F32)).astype(BF16)
    parts = jnp.concatenate([high, middle, low], axis=0)

    counted = lengths[...].astype(F32)
    row64 = lax.broadcasted_iota(jnp.int32, (NSEQ, NSEQ), 0)
    col64 = lax.broadcasted_iota(jnp.int32, (NSEQ, NSEQ), 1)
    upto = jnp.where(row64 <= col64, 1.0, 0.0).astype(BF16)
    wide = jnp.broadcast_to(counted, (8, NSEQ)).astype(BF16)
    ends = jnp.dot(wide, upto, preferred_element_type=F32)[0:1]
    starts = ends - counted
    first_token = ((y * 4 + x) * 8 + z) * TOK
    position = (first_token + lax.broadcasted_iota(jnp.int32, (TOK, NSEQ), 0)).astype(F32)
    inside = jnp.where((position >= starts) & (position < ends), 1.0, 0.0).astype(BF16)
    closing = jnp.max(jnp.where(position + 1.0 == ends, 1.0, 0.0), axis=1, keepdims=True)
    bench_row = lax.broadcasted_iota(jnp.int32, (128, NSEQ), 0)
    table = jnp.where(bench_row == bench[...], 1.0, 0.0).astype(BF16)
    bench_of = lax.dot_general(inside, table, by_rows, preferred_element_type=F32)
    bench_of = bench_of * (1.0 - closing)
    less_one = jnp.broadcast_to(counted - 1.0, (8, NSEQ)).astype(BF16)
    counts = lax.dot_general(less_one, table, by_rows, preferred_element_type=F32)[0:1]

    token_sum = jnp.zeros((TOK, 1), F32)
    for q in range(NQ):
        lanes = pl.ds(q * FQ, FQ)
        for move in returns[q]:
            move.wait_recv()
        back = BACK[:, :, lanes].astype(F32).reshape(NE * CAP, FQ).astype(BF16)
        three = jnp.dot(parts, back, preferred_element_type=F32)
        mixed = (three[0:16] + (three[16:32] + three[32:48])).astype(BF16)
        mixed_out[:, lanes] = mixed
        diff = mixed.astype(F32) - target[:, lanes].astype(F32)
        token_sum += jnp.sum(diff * diff, axis=1, keepdims=True)
    sums = jnp.sum(bench_of * (token_sum / D), axis=0, keepdims=True)

    mine = z * 2 + c
    L1[mine] = jnp.broadcast_to(sums, (8, 128))
    moves = [send(L1.at[mine], L1.at[mine], at(dz=dz, dc=dc)) for dz, dc in column]
    for move in moves:
        move.wait_recv()
    mine = y * 4 + x
    L2[mine] = jnp.sum(L1[...], axis=0)
    moves = [send(L2.at[mine], L2.at[mine], at(dy=dy, dx=dx)) for dy, dx in plane]
    for move in moves:
        move.wait_recv()
    loss_sum = jnp.sum(L2[...], axis=0)[0:1]
    loss_out[...] = (loss_sum / jnp.maximum(counts, 1.0))[:, 0:NB]
    counts_out[...] = counts[:, 0:NB].astype(jnp.int32)
    for copy in started:
        copy.wait_send()


def per_device(tokens, target, router, w_gate, w_up, w_down, expert_ids, lengths, bench_ids):
    vmem = pl.BlockSpec(memory_space=pltpu.VMEM)
    hbm = pl.BlockSpec(memory_space=pl.ANY)
    mixed, loss, counts = pl.pallas_call(
        kernel,
        name="moe",
        out_shape=(
            jax.ShapeDtypeStruct((TOK, DH), BF16),
            jax.ShapeDtypeStruct((1, NB), F32),
            jax.ShapeDtypeStruct((1, NB), jnp.int32),
        ),
        in_specs=[vmem, vmem, vmem, hbm, hbm, hbm, vmem, vmem, vmem],
        out_specs=(vmem, vmem, vmem),
        scratch_shapes=[
            pltpu.VMEM((NE, CAP, DH), BF16),
            pltpu.VMEM((NE, CAP, DH), BF16),
            pltpu.VMEM((4, 2, 128, DH), BF16),
            pltpu.VMEM((4, 2, 128, DH), BF16),
            pltpu.VMEM((2, HID, DH), BF16),
            pltpu.VMEM((2, HID, DH), BF16),
            pltpu.VMEM((2, HID, DH), BF16),
            pltpu.VMEM((256, HID), BF16),
            pltpu.VMEM((4, 256, DH), BF16),
            pltpu.VMEM((4, 256, DH), BF16),
            pltpu.VMEM((4, 256, DH), F32),
            pltpu.VMEM((4, 2, 128, DH), BF16),
            pltpu.VMEM((2, 128, DH), BF16),
            pltpu.VMEM((2, 2, 128, DH), BF16),
            pltpu.VMEM((2, 128, DH), BF16),
            pltpu.VMEM((2, 32, DH), BF16),
            pltpu.VMEM((2, 2, 32, DH), BF16),
            pltpu.VMEM((NE, CAP, DH), BF16),
            pltpu.VMEM((NE, CAP, DH), BF16),
            pltpu.VMEM((TOK, 128), F32),
            pltpu.VMEM((TOK, 128), F32),
            pltpu.VMEM((16, 8, 128), F32),
            pltpu.VMEM((16, 8, 128), F32),
            pltpu.VMEM((8, 128), F32),
            pltpu.SemaphoreType.DMA((6,)),
            pltpu.SemaphoreType.DMA((NSEMS,)),
            pltpu.SemaphoreType.DMA((NSEMS,)),
        ],
        compiler_params=pltpu.CompilerParams(
            collective_id=0, has_side_effects=True, vmem_limit_bytes=66 * 1000 * 1000
        ),
    )(
        tokens, target, router.T, w_gate.swapaxes(1, 2), w_up.swapaxes(1, 2), w_down, expert_ids.T,
        lengths.reshape(1, NSEQ), bench_ids.reshape(1, NSEQ),
    )
    return (mixed, loss.reshape(NB), counts.reshape(NB))


def solution(mesh):
    split = Mesh(
        mesh.devices.reshape(4, 4, mesh.shape["expert"], mesh.shape["tensor"]),
        ("dp_0", "dp_1", "expert", "tensor"),
    )
    in_specs = (
        P(DP_EXPERT, "tensor"),
        P(DP_EXPERT, "tensor"),
        P("tensor", None),
        P("expert", None, DP_TENSOR),
        P("expert", None, DP_TENSOR),
        P("expert", DP_TENSOR, None),
        P(DP_EXPERT, None),
        P(),
        P(),
    )
    out_specs = (P(DP_EXPERT, "tensor"), P(), P())
    return jax.shard_map(
        per_device, mesh=split, in_specs=in_specs, out_specs=out_specs, check_vma=False
    )
```

```python
import jax
import jax.numpy as jnp
from jax import lax
from jax.experimental import pallas as pl
from jax.experimental.pallas import tpu as pltpu
from jax.sharding import Mesh
from jax.sharding import PartitionSpec as P

D = 4096
DH = D // 2
NB = 16
CAP = 8
TOK = 16
HID = 448
NSEQ = 64
NE = 8
NQ = 2
FQ = DH // NQ
DP_EXPERT = ("dp_0", "dp_1", "expert")
DP_TENSOR = ("dp_0", "dp_1", "tensor")
MESH = pl.DeviceIdType.MESH
F32 = jnp.float32
BF16 = jnp.bfloat16
NSEMS = 19 * NQ + 3


def kernel(
    tokens_hbm, target_hbm, router_hbm, wg_hbm, wu_hbm, wd_hbm, ids_hbm, lengths_hbm, bench_hbm,
    mixed_hbm, loss_out, counts_out,
    tokens, target, router, ids, lengths, bench, mixed_out,
    OUT, ZL, XO, XP, WG, WU, WD, H, PX, PR, PO, S, R1, R2, TB, T1, T2, RET, BACK,
    LG, LGR, L1, L2, wsem, ssem, rsem,
):
    y = lax.axis_index("dp_0")
    x = lax.axis_index("dp_1")
    z = lax.axis_index("expert")
    c = lax.axis_index("tensor")

    def at(dy=0, dx=0, dz=0, dc=0):
        return {
            "dp_0": lax.rem(y + dy, 4),
            "dp_1": lax.rem(x + dx, 4),
            "expert": lax.rem(z + dz, 8),
            "tensor": lax.rem(c + dc, 2),
        }

    column = [(dz, dc) for dz in range(8) for dc in range(2)][1:]
    plane = [(dy, dx) for dy in range(4) for dx in range(4)][1:]
    barrier = pltpu.get_barrier_semaphore()
    for dz, dc in column:
        pl.semaphore_signal(barrier, inc=1, device_id=at(dz=dz, dc=dc), device_id_type=MESH)
    for dy, dx in plane:
        pl.semaphore_signal(barrier, inc=1, device_id=at(dy=dy, dx=dx), device_id_type=MESH)

    inputs = (
        (ids_hbm, ids), (tokens_hbm, tokens), (router_hbm, router),
        (target_hbm, target), (lengths_hbm, lengths), (bench_hbm, bench),
    )
    inputs = [pltpu.make_async_copy(src, dst, wsem.at[6 + i]) for i, (src, dst) in enumerate(inputs)]
    for copy in inputs:
        copy.start()
    loads = []
    for half in range(2):
        first = pl.multiple_of(lax.rem(c + half, 2) * DH, DH)
        loads.append(pltpu.make_async_copy(wg_hbm.at[0, :, pl.ds(first, DH)], WG.at[half], wsem.at[3 * half]))
        loads.append(pltpu.make_async_copy(wu_hbm.at[0, :, pl.ds(first, DH)], WU.at[half], wsem.at[3 * half + 1]))
        loads.append(pltpu.make_async_copy(wd_hbm.at[0, :, pl.ds(first, DH)], WD.at[half], wsem.at[3 * half + 2]))
    for load in loads:
        load.start()

    waits, numbers = [], {}

    def send(group, src, dst, device):
        number = numbers.setdefault(group, len(numbers))
        pltpu.make_async_remote_copy(
            src_ref=src, dst_ref=dst, send_sem=ssem.at[number], recv_sem=rsem.at[number],
            device_id=device, device_id_type=MESH,
        ).start()

    def arrived(group, region):
        number = numbers[group]
        copies = pltpu.make_async_remote_copy(
            src_ref=region, dst_ref=region, send_sem=ssem.at[number], recv_sem=rsem.at[number],
            device_id=at(dc=1), device_id_type=MESH,
        )
        copies.wait_recv()
        waits.append(copies)

    for copy in inputs:
        copy.wait()
    lane = lax.broadcasted_iota(jnp.int32, (TOK, 128), 1)
    row16 = lax.broadcasted_iota(jnp.int32, (TOK, TOK), 0)
    col16 = lax.broadcasted_iota(jnp.int32, (TOK, TOK), 1)

    def as_column(row):
        spread = jnp.broadcast_to(row.astype(F32), (TOK, TOK))
        return jnp.sum(jnp.where(row16 == col16, spread, 0.0), axis=1, keepdims=True).astype(jnp.int32)

    id_0 = as_column(ids[0:1, :])
    id_1 = as_column(ids[1:2, :])
    marks_0 = jnp.where(lane == id_0, 1.0, 0.0)
    marks_1 = jnp.where(lane == id_1, 1.0, 0.0)
    earlier = jnp.where(col16 < row16, 1.0, 0.0).astype(BF16)
    before = jnp.dot(earlier, (marks_0 + marks_1).astype(BF16), preferred_element_type=F32)
    slot_0 = jnp.sum(before * marks_0, axis=1, keepdims=True)
    slot_1 = jnp.sum(before * marks_1, axis=1, keepdims=True)
    place_0 = (((id_0 - z + NE) & (NE - 1)) * CAP).astype(F32) + slot_0
    place_1 = (((id_1 - z + NE) & (NE - 1)) * CAP).astype(F32) + slot_1
    place = lax.broadcasted_iota(jnp.int32, (TOK, NE * CAP), 1).astype(F32)
    put_0 = jnp.where(place == place_0, 1.0, 0.0)
    put_1 = jnp.where(place == place_1, 1.0, 0.0)
    dispatch = (put_0 + put_1).astype(BF16)
    for q in range(NQ):
        lanes = pl.ds(q * FQ, FQ)
        rows = lax.dot_general(
            dispatch, tokens[:, lanes], (((0,), (0,)), ((), ())), preferred_element_type=F32
        )
        rows = rows.reshape(NE, CAP, FQ).astype(BF16)
        OUT[:, :, lanes] = rows
        ZL[0, :, lanes] = rows[0]
    by_rows = (((1,), (1,)), ((), ()))
    partial = lax.dot_general(tokens[...], router[...], by_rows, preferred_element_type=F32)
    LG[...] = jnp.zeros((TOK, 128), F32)
    LG[:, 0:NE] = partial

    pl.semaphore_wait(barrier, len(column) + len(plane))

    for q in range(NQ):
        lanes = pl.ds(q * FQ, FQ)
        for j in (4, 3, 5, 2, 6, 1, 7):
            send(("z", q), OUT.at[j, :, lanes], ZL.at[8 - j, :, lanes], at(dz=j))
    send("logits", LG, LGR, at(dc=1))

    def small_axis(ab, step):
        return at(dx=step) if ab == 0 else at(dy=step)

    def large_axis(ab, step):
        return at(dy=step) if ab == 0 else at(dx=step)

    def wavefront(stages, lags):
        for tick in range(NQ + lags[-1]):
            for stage, lag in zip(stages, lags):
                if 0 <= tick - lag < NQ:
                    stage(tick - lag, pl.ds((tick - lag) * FQ, FQ))

    def from_z(q, lanes):
        arrived(("z", q), ZL.at[1:8, :, lanes])
        for ab in range(2):
            rows = ZL[4 * ab : 4 * ab + 4, :, lanes].astype(F32).reshape(32, FQ)
            XO[0, ab, 0:32, lanes] = rows.astype(BF16)
            src = XO.at[0, ab, 0:32, lanes]
            send(("near_small", q), src, XO.at[0, ab, 96:128, lanes], small_axis(ab, 1))
            send(("near_small", q), src, XO.at[0, ab, 32:64, lanes], small_axis(ab, 3))

    def small_forward(q, lanes):
        arrived(("near_small", q), XO.at[0, :, 0:64, lanes])
        for ab in range(2):
            send(
                ("far_small", q), XO.at[0, ab, 96:112, lanes], XO.at[0, ab, 64:80, lanes], small_axis(ab, 1)
            )
            send(
                ("far_small", q), XO.at[0, ab, 48:64, lanes], XO.at[0, ab, 80:96, lanes], small_axis(ab, 3)
            )

    def to_partner(unit, q, lanes):
        send(("across", unit, q), XO.at[unit, :, :, lanes], XP.at[unit, :, :, lanes], at(dc=1))

    def large_own(q, lanes):
        arrived(("far_small", q), XO.at[0, :, 0:32, lanes])
        for ab in range(2):
            upper, lower = XO.at[0, ab, 0:64, lanes], XO.at[0, ab, 64:128, lanes]
            send(("near", q), upper, XO.at[1, ab, 0:64, lanes], large_axis(ab, 1))
            send(("near", q), lower, XO.at[1, ab, 64:128, lanes], large_axis(ab, 3))
        to_partner(0, q, lanes)

    def large_forward(q, lanes):
        arrived(("near", q), XO.at[1, :, :, lanes])
        for ab in range(2):
            send(("far", q), XO.at[1, ab, 0:64, lanes], XO.at[2, ab, 0:64, lanes], large_axis(ab, 1))
            send(("far", q), XO.at[1, ab, 64:128, lanes], XO.at[2, ab, 64:128, lanes], large_axis(ab, 3))
        to_partner(1, q, lanes)

    wavefront((from_z, small_forward, large_own), (0, 1, 2))
    halves = [(q, pl.ds(q * FQ, FQ)) for q in range(NQ)]
    large_forward(*halves[0])

    for load in loads:
        load.wait()

    def up(unit):
        for q, lanes in halves:
            arrived(("across", unit, q), XP.at[unit, :, :, lanes])
        own = XO[unit].reshape(256, DH)
        other = XP[unit].reshape(256, DH)
        gate = lax.dot_general(WG[0], own, by_rows, preferred_element_type=F32)
        gate += lax.dot_general(WG[1], other, by_rows, preferred_element_type=F32)
        raise_ = lax.dot_general(WU[0], own, by_rows, preferred_element_type=F32)
        raise_ += lax.dot_general(WU[1], other, by_rows, preferred_element_type=F32)
        H[...] = (gate * jax.nn.sigmoid(gate) * raise_).astype(BF16).T

    def down(unit):
        for q, lanes in halves:
            for n in range(q * FQ, q * FQ + FQ, 512):
                cols = slice(n, n + 512)
                PX[unit, :, cols] = jnp.dot(H[...], WD[1, :, cols], preferred_element_type=F32).astype(BF16)
            send(("sums", unit, q), PX.at[unit, :, lanes], PR.at[unit, :, lanes], at(dc=1))
        for n in range(0, DH, 512):
            cols = slice(n, n + 512)
            PO[unit, :, cols] = jnp.dot(H[...], WD[0, :, cols], preferred_element_type=F32)

    def chip_sum(unit, q, lanes):
        arrived(("sums", unit, q), PR.at[unit, :, lanes])
        return PO[unit, :, lanes] + PR[unit, :, lanes].astype(F32)

    up(0)
    large_forward(*halves[1])
    for q, lanes in halves:
        for ab in range(2):
            upper, lower = XO.at[0, ab, 0:64, lanes], XO.at[0, ab, 64:128, lanes]
            send(("late", q), lower, XO.at[3, ab, 64:128, lanes], large_axis(ab, 1))
            send(("late", q), upper, XO.at[3, ab, 0:64, lanes], large_axis(ab, 3))
    down(0)
    up(1)
    down(1)
    for q, lanes in halves:
        arrived(("far", q), XO.at[2, :, :, lanes])
        to_partner(2, q, lanes)
    for q, lanes in halves:
        S[0, :, :, lanes] = chip_sum(1, q, lanes).astype(BF16).reshape(2, 128, FQ)
        for ab in range(2):
            send(("sent", q), S.at[0, ab, 64:128, lanes], R2.at[0, ab, 64:128, lanes], large_axis(ab, 1))
            send(("sent", q), S.at[0, ab, 0:64, lanes], R2.at[1, ab, 0:64, lanes], large_axis(ab, 3))
    up(2)
    for q, lanes in halves:
        arrived(("late", q), XO.at[3, :, :, lanes])
        to_partner(3, q, lanes)
    down(2)
    for q, lanes in halves:
        S[1, :, :, lanes] = chip_sum(2, q, lanes).astype(BF16).reshape(2, 128, FQ)
        for ab in range(2):
            send(("first", q), S.at[1, ab, 0:64, lanes], R1.at[ab, 0:64, lanes], large_axis(ab, 1))
            send(("first", q), S.at[1, ab, 64:128, lanes], R1.at[ab, 64:128, lanes], large_axis(ab, 3))
    up(3)
    down(3)
    arrived("logits", LGR)
    logits = LG[...] + LGR[...]
    picked_0 = jnp.sum(logits * marks_0, axis=1, keepdims=True)
    picked_1 = jnp.sum(logits * marks_1, axis=1, keepdims=True)
    gate_0 = jax.nn.sigmoid(picked_0 - picked_1)
    gate_1 = jax.nn.sigmoid(picked_1 - picked_0)
    weights = gate_0 * put_0 + gate_1 * put_1
    high = weights.astype(BF16)
    rest = weights - high.astype(F32)
    middle = rest.astype(BF16)
    low = (rest - middle.astype(F32)).astype(BF16)
    parts = jnp.concatenate([high, middle, low], axis=0)

    counted = lengths[...].astype(F32)
    row64 = lax.broadcasted_iota(jnp.int32, (NSEQ, NSEQ), 0)
    col64 = lax.broadcasted_iota(jnp.int32, (NSEQ, NSEQ), 1)
    upto = jnp.where(row64 <= col64, 1.0, 0.0).astype(BF16)
    wide = jnp.broadcast_to(counted, (8, NSEQ)).astype(BF16)
    ends = jnp.dot(wide, upto, preferred_element_type=F32)[0:1]
    starts = ends - counted
    first_token = ((y * 4 + x) * 8 + z) * TOK
    position = (first_token + lax.broadcasted_iota(jnp.int32, (TOK, NSEQ), 0)).astype(F32)
    inside = jnp.where((position >= starts) & (position < ends), 1.0, 0.0).astype(BF16)
    closing = jnp.max(jnp.where(position + 1.0 == ends, 1.0, 0.0), axis=1, keepdims=True)
    bench_row = lax.broadcasted_iota(jnp.int32, (128, NSEQ), 0)
    table = jnp.where(bench_row == bench[...], 1.0, 0.0).astype(BF16)
    bench_of = lax.dot_general(inside, table, by_rows, preferred_element_type=F32)
    bench_of = bench_of * (1.0 - closing)
    less_one = jnp.broadcast_to(counted - 1.0, (8, NSEQ)).astype(BF16)
    counts = lax.dot_general(less_one, table, by_rows, preferred_element_type=F32)[0:1]

    for q, lanes in halves:
        total = chip_sum(3, q, lanes)
        arrived(("first", q), R1.at[:, :, lanes])
        S[2, :, :, lanes] = (total.reshape(2, 128, FQ) + R1[:, :, lanes].astype(F32)).astype(BF16)
        for ab in range(2):
            send(("sent", q), S.at[2, ab, 0:64, lanes], R2.at[0, ab, 0:64, lanes], large_axis(ab, 1))
            send(("sent", q), S.at[2, ab, 64:128, lanes], R2.at[1, ab, 64:128, lanes], large_axis(ab, 3))
    for q, lanes in halves:
        PO[0, :, lanes] = chip_sum(0, q, lanes)
    token_sums = []

    def large_total(q, lanes):
        arrived(("sent", q), R2.at[:, :, :, lanes])
        for ab in range(2):
            block = slice(128 * ab, 128 * ab + 128)
            total = PO[0, block, lanes] + R2[0, ab, :, lanes].astype(F32)
            total += R2[1, ab, :, lanes].astype(F32)
            PO[0, block, lanes] = total
            TB[ab, :, lanes] = total.astype(BF16)
            send(("first_small", q), TB.at[ab, 64:80, lanes], T1.at[ab, 0:16, lanes], small_axis(ab, 1))
            send(("first_small", q), TB.at[ab, 80:96, lanes], T1.at[ab, 16:32, lanes], small_axis(ab, 3))
            send(("sent_small", q), TB.at[ab, 48:64, lanes], T2.at[0, ab, 16:32, lanes], small_axis(ab, 1))
            send(("sent_small", q), TB.at[ab, 96:112, lanes], T2.at[1, ab, 0:16, lanes], small_axis(ab, 3))

    def small_step(q, lanes):
        arrived(("first_small", q), T1.at[:, :, lanes])
        for ab in range(2):
            for rel, base, half, slot in ((1, 32, slice(0, 16), 0), (3, 96, slice(16, 32), 1)):
                rows = slice(base + half.start, base + half.stop)
                TB[ab, rows, lanes] = (
                    PO[0, 128 * ab + rows.start : 128 * ab + rows.stop, lanes] + T1[ab, half, lanes].astype(F32)
                ).astype(BF16)
                send(
                    ("sent_small", q), TB.at[ab, rows, lanes], T2.at[slot, ab, half, lanes], small_axis(ab, rel)
                )

    def small_total(q, lanes):
        arrived(("sent_small", q), T2.at[:, :, :, lanes])
        for ab in range(2):
            total = PO[0, 128 * ab : 128 * ab + 32, lanes]
            total += T2[0, ab, :, lanes].astype(F32)
            total += T2[1, ab, :, lanes].astype(F32)
            RET[4 * ab : 4 * ab + 4, :, lanes] = total.reshape(4, CAP, FQ).astype(BF16)
        BACK[0, :, lanes] = RET[0, :, lanes]
        for j in (4, 3, 5, 2, 6, 1, 7):
            send(("back", q), RET.at[j, :, lanes], BACK.at[8 - j, :, lanes], at(dz=j))

    def mix(q, lanes):
        arrived(("back", q), BACK.at[1:8, :, lanes])
        back = BACK[:, :, lanes].astype(F32).reshape(NE * CAP, FQ).astype(BF16)
        three = jnp.dot(parts, back, preferred_element_type=F32)
        mixed = (three[0:16] + (three[16:32] + three[32:48])).astype(BF16)
        mixed_out[:, lanes] = mixed
        diff = mixed.astype(F32) - target[:, lanes].astype(F32)
        token_sums.append(jnp.sum(diff * diff, axis=1, keepdims=True))

    wavefront((large_total, small_step, small_total, mix), (0, 1, 2, 4))
    token_sum = sum(token_sums[1:], token_sums[0])
    sums = jnp.sum(bench_of * (token_sum / D), axis=0, keepdims=True)

    hand = pltpu.make_async_copy(mixed_out, mixed_hbm, wsem.at[12])
    hand.start()
    mine = z * 2 + c
    L1[mine] = sums
    for dz, dc in column:
        send("column", L1.at[mine], L1.at[mine], at(dz=dz, dc=dc))
    arrived("column", L1.at[0:15])
    mine = y * 4 + x
    L2[mine] = jnp.sum(L1[...], axis=0)
    for dy, dx in plane:
        send("plane", L2.at[mine], L2.at[mine], at(dy=dy, dx=dx))
    arrived("plane", L2.at[0:15])
    loss_sum = jnp.sum(L2[...], axis=0)
    loss_out[...] = (loss_sum / jnp.maximum(counts, 1.0))[:, 0:NB]
    counts_out[...] = counts[:, 0:NB].astype(jnp.int32)
    hand.wait()
    for copy in waits:
        copy.wait_send()


def hand_over(*refs):
    sources, targets, stages, sems = refs[0:3], refs[3:6], refs[6:9], refs[9]
    arriving = [pltpu.make_async_copy(sources[i], stages[i], sems.at[i]) for i in range(3)]
    leaving = [pltpu.make_async_copy(stages[i], targets[i], sems.at[3 + i]) for i in range(3)]
    for copy in arriving:
        copy.start()
    for i in range(3):
        arriving[i].wait()
        leaving[i].start()
    for copy in leaving:
        copy.wait()


def per_device(tokens, target, router, w_gate, w_up, w_down, expert_ids, lengths, bench_ids):
    vmem = pl.BlockSpec(memory_space=pltpu.VMEM)
    hbm = pl.BlockSpec(memory_space=pltpu.HBM)
    mixed, loss, counts = pl.pallas_call(
        kernel,
        name="moe",
        out_shape=(
            jax.ShapeDtypeStruct((TOK, DH), BF16),
            jax.ShapeDtypeStruct((1, NB), F32),
            jax.ShapeDtypeStruct((1, NB), jnp.int32),
        ),
        in_specs=[hbm] * 9,
        out_specs=(hbm, vmem, vmem),
        scratch_shapes=[
            pltpu.VMEM((TOK, DH), BF16),
            pltpu.VMEM((TOK, DH), BF16),
            pltpu.VMEM((NE, DH), BF16),
            pltpu.VMEM((2, TOK), jnp.int32),
            pltpu.VMEM((1, NSEQ), jnp.int32),
            pltpu.VMEM((1, NSEQ), jnp.int32),
            pltpu.VMEM((TOK, DH), BF16),
            pltpu.VMEM((NE, CAP, DH), BF16),
            pltpu.VMEM((NE, CAP, DH), BF16),
            pltpu.VMEM((4, 2, 128, DH), BF16),
            pltpu.VMEM((4, 2, 128, DH), BF16),
            pltpu.VMEM((2, HID, DH), BF16),
            pltpu.VMEM((2, HID, DH), BF16),
            pltpu.VMEM((2, HID, DH), BF16),
            pltpu.VMEM((256, HID), BF16),
            pltpu.VMEM((4, 256, DH), BF16),
            pltpu.VMEM((4, 256, DH), BF16),
            pltpu.VMEM((4, 256, DH), F32),
            pltpu.VMEM((3, 2, 128, DH), BF16),
            pltpu.VMEM((2, 128, DH), BF16),
            pltpu.VMEM((2, 2, 128, DH), BF16),
            pltpu.VMEM((2, 128, DH), BF16),
            pltpu.VMEM((2, 32, DH), BF16),
            pltpu.VMEM((2, 2, 32, DH), BF16),
            pltpu.VMEM((NE, CAP, DH), BF16),
            pltpu.VMEM((NE, CAP, DH), BF16),
            pltpu.VMEM((TOK, 128), F32),
            pltpu.VMEM((TOK, 128), F32),
            pltpu.VMEM((16, 1, 128), F32),
            pltpu.VMEM((16, 1, 128), F32),
            pltpu.SemaphoreType.DMA((13,)),
            pltpu.SemaphoreType.DMA((NSEMS,)),
            pltpu.SemaphoreType.DMA((NSEMS,)),
        ],
        compiler_params=pltpu.CompilerParams(
            collective_id=0, has_side_effects=True, vmem_limit_bytes=66 * 1000 * 1000
        ),
    )(
        tokens, target, router.T, w_gate.swapaxes(1, 2), w_up.swapaxes(1, 2), w_down, expert_ids.T,
        lengths.reshape(1, NSEQ), bench_ids.reshape(1, NSEQ),
    )
    mixed, loss, counts = pl.pallas_call(
        hand_over,
        name="hand_over",
        out_shape=(
            jax.ShapeDtypeStruct((TOK, DH), BF16),
            jax.ShapeDtypeStruct((1, NB), F32),
            jax.ShapeDtypeStruct((1, NB), jnp.int32),
        ),
        in_specs=[hbm, hbm, hbm],
        out_specs=(hbm, hbm, hbm),
        scratch_shapes=[
            pltpu.VMEM((TOK, DH), BF16),
            pltpu.VMEM((1, NB), F32),
            pltpu.VMEM((1, NB), jnp.int32),
            pltpu.SemaphoreType.DMA((6,)),
        ],
        compiler_params=pltpu.CompilerParams(vmem_limit_bytes=66 * 1000 * 1000),
    )(mixed, loss, counts)
    return (mixed, loss.reshape(NB), counts.reshape(NB))


def solution(mesh):
    split = Mesh(
        mesh.devices.reshape(4, 4, mesh.shape["expert"], mesh.shape["tensor"]),
        ("dp_0", "dp_1", "expert", "tensor"),
    )
    in_specs = (
        P(DP_EXPERT, "tensor"),
        P(DP_EXPERT, "tensor"),
        P("tensor", None),
        P("expert", None, DP_TENSOR),
        P("expert", None, DP_TENSOR),
        P("expert", DP_TENSOR, None),
        P(DP_EXPERT, None),
        P(),
        P(),
    )
    out_specs = (P(DP_EXPERT, "tensor"), P(), P())
    return jax.shard_map(
        per_device, mesh=split, in_specs=in_specs, out_specs=out_specs, check_vma=False
    )
```

```python
import jax
import jax.numpy as jnp
from jax import lax
from jax.experimental import pallas as pl
from jax.experimental.pallas import tpu as pltpu
from jax.sharding import Mesh
from jax.sharding import PartitionSpec as P

D = 4096
DH = D // 2
NB = 16
CAP = 8
TOK = 16
HID = 448
NSEQ = 64
NE = 8
NQ = 2
FQ = DH // NQ
DP_EXPERT = ("dp_0", "dp_1", "expert")
DP_TENSOR = ("dp_0", "dp_1", "tensor")
MESH = pl.DeviceIdType.MESH
F32 = jnp.float32
BF16 = jnp.bfloat16
NSEMS = 46


def kernel(
    tokens_hbm, target_hbm, router_hbm, wg_hbm, wu_hbm, wd_hbm, ids_hbm, lengths_hbm, bench_hbm,
    mixed_out, loss_out, counts_out,
    tokens, target, router, ids, lengths, bench,
    OUT, ZL, ZR, XO, XP, WG, WU, WD, G, H, PX, PR, PO, S, R1, R2, TB, T1, T2, RET, BACK,
    LG, LGR, L1, L2, wsem, ssem, rsem,
):
    y = lax.axis_index("dp_0")
    x = lax.axis_index("dp_1")
    z = lax.axis_index("expert")
    c = lax.axis_index("tensor")

    def at(dy=0, dx=0, dz=0, dc=0):
        return {
            "dp_0": lax.rem(y + dy, 4),
            "dp_1": lax.rem(x + dx, 4),
            "expert": lax.rem(z + dz, 8),
            "tensor": lax.rem(c + dc, 2),
        }

    column = [(dz, dc) for dz in range(8) for dc in range(2)][1:]
    plane = [(dy, dx) for dy in range(4) for dx in range(4)][1:]
    barrier = pltpu.get_barrier_semaphore()
    for dz, dc in column:
        pl.semaphore_signal(barrier, inc=1, device_id=at(dz=dz, dc=dc), device_id_type=MESH)
    for dy, dx in plane:
        pl.semaphore_signal(barrier, inc=1, device_id=at(dy=dy, dx=dx), device_id_type=MESH)

    inputs = (
        (ids_hbm, ids), (tokens_hbm, tokens), (router_hbm, router),
        (target_hbm, target), (lengths_hbm, lengths), (bench_hbm, bench),
    )
    inputs = [pltpu.make_async_copy(src, dst, wsem.at[6 + i]) for i, (src, dst) in enumerate(inputs)]
    for copy in inputs:
        copy.start()
    loads = []
    for half in range(2):
        first = pl.multiple_of(lax.rem(c + half, 2) * DH, DH)
        loads.append(pltpu.make_async_copy(wg_hbm.at[0, :, pl.ds(first, DH)], WG.at[half], wsem.at[3 * half]))
        loads.append(pltpu.make_async_copy(wu_hbm.at[0, :, pl.ds(first, DH)], WU.at[half], wsem.at[3 * half + 1]))
        loads.append(pltpu.make_async_copy(wd_hbm.at[0, :, pl.ds(first, DH)], WD.at[half], wsem.at[3 * half + 2]))
    for load in loads:
        load.start()

    waits, numbers = [], {}

    def send(group, src, dst, device):
        number = numbers.setdefault(group, len(numbers))
        pltpu.make_async_remote_copy(
            src_ref=src, dst_ref=dst, send_sem=ssem.at[number], recv_sem=rsem.at[number],
            device_id=device, device_id_type=MESH,
        ).start()

    def arrived(group, region):
        number = numbers[group]
        copies = pltpu.make_async_remote_copy(
            src_ref=region, dst_ref=region, send_sem=ssem.at[number], recv_sem=rsem.at[number],
            device_id=at(dc=1), device_id_type=MESH,
        )
        copies.wait_recv()
        waits.append(copies)

    for copy in inputs:
        copy.wait()
    lane = lax.broadcasted_iota(jnp.int32, (TOK, 128), 1)
    row16 = lax.broadcasted_iota(jnp.int32, (TOK, TOK), 0)
    col16 = lax.broadcasted_iota(jnp.int32, (TOK, TOK), 1)

    def as_column(row):
        spread = jnp.broadcast_to(row.astype(F32), (TOK, TOK))
        return jnp.sum(jnp.where(row16 == col16, spread, 0.0), axis=1, keepdims=True).astype(jnp.int32)

    id_0 = as_column(ids[0:1, :])
    id_1 = as_column(ids[1:2, :])
    marks_0 = jnp.where(lane == id_0, 1.0, 0.0)
    marks_1 = jnp.where(lane == id_1, 1.0, 0.0)
    earlier = jnp.where(col16 < row16, 1.0, 0.0).astype(BF16)
    before = jnp.dot(earlier, (marks_0 + marks_1).astype(BF16), preferred_element_type=F32)
    slot_0 = jnp.sum(before * marks_0, axis=1, keepdims=True)
    slot_1 = jnp.sum(before * marks_1, axis=1, keepdims=True)
    place_0 = (((id_0 - z + NE) & (NE - 1)) * CAP).astype(F32) + slot_0
    place_1 = (((id_1 - z + NE) & (NE - 1)) * CAP).astype(F32) + slot_1
    place = lax.broadcasted_iota(jnp.int32, (TOK, NE * CAP), 1).astype(F32)
    put_0 = jnp.where(place == place_0, 1.0, 0.0)
    put_1 = jnp.where(place == place_1, 1.0, 0.0)
    dispatch = (put_0 + put_1).astype(BF16)
    for q in range(NQ):
        lanes = pl.ds(q * FQ, FQ)
        rows = lax.dot_general(
            dispatch, tokens[:, lanes], (((0,), (0,)), ((), ())), preferred_element_type=F32
        )
        rows = rows.reshape(NE, CAP, FQ).astype(BF16)
        OUT[:, :, lanes] = rows
        ZL[0, :, lanes] = rows[0]
    by_rows = (((1,), (1,)), ((), ()))
    partial = lax.dot_general(tokens[...], router[...], by_rows, preferred_element_type=F32)
    LG[...] = jnp.zeros((TOK, 128), F32)
    LG[:, 0:NE] = partial

    pl.semaphore_wait(barrier, len(column) + len(plane))

    for q in range(NQ):
        lanes = pl.ds(q * FQ, FQ)
        for j in (4, 3, 5, 2, 6, 1, 7):
            send(("z", q), OUT.at[j, :, lanes], ZL.at[8 - j, :, lanes], at(dz=j))
    send("logits", LG, LGR, at(dc=1))

    def small_axis(ab, step):
        return at(dx=step) if ab == 0 else at(dy=step)

    def large_axis(ab, step):
        return at(dy=step) if ab == 0 else at(dx=step)

    def wavefront(stages, lags):
        for tick in range(NQ + lags[-1]):
            for stage, lag in zip(stages, lags):
                if 0 <= tick - lag < NQ:
                    stage(tick - lag, pl.ds((tick - lag) * FQ, FQ))

    def from_z(q, lanes):
        arrived(("z", q), ZL.at[1:8, :, lanes])
        for ab in range(2):
            rows = ZL[4 * ab : 4 * ab + 4, :, lanes].astype(F32).reshape(32, FQ).astype(BF16)
            ZR[ab, :, lanes] = rows
            XO[0, ab, 0:16, lanes] = rows[0:16]
            XO[0, ab, 112:128, lanes] = rows[16:32]
        for ab in range(2):
            src = ZR.at[ab, :, lanes]
            send(("near_small", q), src, XO.at[0, ab, 80:112, lanes], small_axis(ab, 1))
            send(("near_small", q), src, XO.at[0, ab, 16:48, lanes], small_axis(ab, 3))
        for ab in range(2):
            early(q, lanes, ab, 0, 16)

    def early(q, lanes, ab, start, stop):
        for rows, step in ((slice(start, stop), 1), (slice(128 - stop, 128 - start), 3)):
            send(("near", q), XO.at[0, ab, rows, lanes], XO.at[1, ab, rows, lanes], large_axis(ab, step))

    def small_forward(q, lanes):
        arrived(("near_small", q), XO.at[0, :, 0:64, lanes])
        for ab in range(2):
            send(
                ("far_small", q), XO.at[0, ab, 80:96, lanes], XO.at[0, ab, 48:64, lanes], small_axis(ab, 1)
            )
            send(
                ("far_small", q), XO.at[0, ab, 32:48, lanes], XO.at[0, ab, 64:80, lanes], small_axis(ab, 3)
            )
        for ab in range(2):
            early(q, lanes, ab, 16, 48)

    def to_partner(unit, q, lanes):
        send(("across", unit, q), XO.at[unit, :, :, lanes], XP.at[unit, :, :, lanes], at(dc=1))

    def large_own(q, lanes):
        arrived(("far_small", q), XO.at[0, :, 0:32, lanes])
        for ab in range(2):
            early(q, lanes, ab, 48, 64)
        to_partner(0, q, lanes)
        if q == 0:
            late(0, lanes, 0, 32)

    def large_forward(q, lanes):
        arrived(("near", q), XO.at[1, :, :, lanes])
        for ab in range(2):
            send(("far", q), XO.at[1, ab, 0:64, lanes], XO.at[2, ab, 0:64, lanes], large_axis(ab, 1))
            send(("far", q), XO.at[1, ab, 64:128, lanes], XO.at[2, ab, 64:128, lanes], large_axis(ab, 3))
        to_partner(1, q, lanes)

    def late(q, lanes, lower, upper):
        for ab in range(2):
            for rows, step in ((slice(128 - upper, 128 - lower), 1), (slice(lower, upper), 3)):
                send(("late", q), XO.at[0, ab, rows, lanes], XO.at[3, ab, rows, lanes], large_axis(ab, step))

    wavefront((from_z, small_forward, large_own), (0, 1, 2))
    halves = [(q, pl.ds(q * FQ, FQ)) for q in range(NQ)]

    def up_own(unit):
        own = XO[unit].reshape(256, DH)
        G[0] = lax.dot_general(WG[0], own, by_rows, preferred_element_type=F32)
        G[1] = lax.dot_general(WU[0], own, by_rows, preferred_element_type=F32)

    def up_other(unit):
        for q, lanes in halves:
            arrived(("across", unit, q), XP.at[unit, :, :, lanes])
        other = XP[unit].reshape(256, DH)
        gate = G[0] + lax.dot_general(WG[1], other, by_rows, preferred_element_type=F32)
        raise_ = G[1] + lax.dot_general(WU[1], other, by_rows, preferred_element_type=F32)
        H[...] = (gate * jax.nn.sigmoid(gate) * raise_).astype(BF16).T

    def down(unit, between=None):
        for q, lanes in halves:
            for n in range(q * FQ, q * FQ + FQ, 512):
                cols = slice(n, n + 512)
                PX[unit, :, cols] = jnp.dot(H[...], WD[1, :, cols], preferred_element_type=F32).astype(BF16)
            send(("sums", unit, q), PX.at[unit, :, lanes], PR.at[unit, :, lanes], at(dc=1))
        if between is not None:
            between()
        for n in range(0, DH, 512):
            cols = slice(n, n + 512)
            PO[unit, :, cols] = jnp.dot(H[...], WD[0, :, cols], preferred_element_type=F32)

    def chip_sum(unit, q, lanes):
        arrived(("sums", unit, q), PR.at[unit, :, lanes])
        return PO[unit, :, lanes] + PR[unit, :, lanes].astype(F32)

    for load in loads:
        load.wait()
    up_own(0)
    large_forward(*halves[0])
    up_other(0)
    large_forward(*halves[1])
    late(*halves[0], 32, 64)
    late(*halves[1], 0, 64)
    down(0)
    up_own(1)
    up_other(1)
    down(1)
    for q, lanes in halves:
        arrived(("far", q), XO.at[2, :, :, lanes])
        to_partner(2, q, lanes)
    up_own(2)
    for q, lanes in halves:
        S[0, :, :, lanes] = chip_sum(1, q, lanes).astype(BF16).reshape(2, 128, FQ)
        for ab in range(2):
            send("direct", S.at[0, ab, 64:128, lanes], R2.at[0, ab, 64:128, lanes], large_axis(ab, 1))
            send("direct", S.at[0, ab, 0:64, lanes], R2.at[1, ab, 0:64, lanes], large_axis(ab, 3))
    up_other(2)
    def last_block():
        for q, lanes in halves:
            arrived(("late", q), XO.at[3, :, :, lanes])
            to_partner(3, q, lanes)

    down(2, last_block)
    up_own(3)
    parts_of = ((48, 64), (16, 48), (0, 16))
    for q, lanes in halves:
        S[1, :, :, lanes] = chip_sum(2, q, lanes).astype(BF16).reshape(2, 128, FQ)
    for part, (start, stop) in enumerate(parts_of):
        for ab in range(2):
            for rows, step in ((slice(start, stop), 1), (slice(128 - stop, 128 - start), 3)):
                send(("first", part), S.at[1, ab, rows], R1.at[ab, rows], large_axis(ab, step))
    up_other(3)
    down(3)
    arrived("logits", LGR)
    logits = LG[...] + LGR[...]
    picked_0 = jnp.sum(logits * marks_0, axis=1, keepdims=True)
    picked_1 = jnp.sum(logits * marks_1, axis=1, keepdims=True)
    gate_0 = jax.nn.sigmoid(picked_0 - picked_1)
    gate_1 = jax.nn.sigmoid(picked_1 - picked_0)
    weights = gate_0 * put_0 + gate_1 * put_1
    high = weights.astype(BF16)
    rest = weights - high.astype(F32)
    middle = rest.astype(BF16)
    low = (rest - middle.astype(F32)).astype(BF16)
    parts = jnp.concatenate([high, middle, low], axis=0)

    counted = lengths[...].astype(F32)
    row64 = lax.broadcasted_iota(jnp.int32, (NSEQ, NSEQ), 0)
    col64 = lax.broadcasted_iota(jnp.int32, (NSEQ, NSEQ), 1)
    upto = jnp.where(row64 <= col64, 1.0, 0.0).astype(BF16)
    wide = jnp.broadcast_to(counted, (8, NSEQ)).astype(BF16)
    ends = jnp.dot(wide, upto, preferred_element_type=F32)[0:1]
    starts = ends - counted
    first_token = ((y * 4 + x) * 8 + z) * TOK
    position = (first_token + lax.broadcasted_iota(jnp.int32, (TOK, NSEQ), 0)).astype(F32)
    inside = jnp.where((position >= starts) & (position < ends), 1.0, 0.0).astype(BF16)
    closing = jnp.max(jnp.where(position + 1.0 == ends, 1.0, 0.0), axis=1, keepdims=True)
    bench_row = lax.broadcasted_iota(jnp.int32, (128, NSEQ), 0)
    table = jnp.where(bench_row == bench[...], 1.0, 0.0).astype(BF16)
    bench_of = lax.dot_general(inside, table, by_rows, preferred_element_type=F32)
    bench_of = bench_of * (1.0 - closing)
    less_one = jnp.broadcast_to(counted - 1.0, (8, NSEQ)).astype(BF16)
    counts = lax.dot_general(less_one, table, by_rows, preferred_element_type=F32)[0:1]

    for q, lanes in halves:
        PO[0, :, lanes] = chip_sum(0, q, lanes)
    for q, lanes in halves:
        PO[3, :, lanes] = chip_sum(3, q, lanes)
    def second(part):
        start, stop = parts_of[part]
        arrived(("first", part), R1.at[:, 0 : 2 * (stop - start)])
        for ab in range(2):
            for slot, rows, step in ((0, slice(start, stop), 1), (1, slice(128 - stop, 128 - start), 3)):
                mine = slice(128 * ab + rows.start, 128 * ab + rows.stop)
                S[2, ab, rows] = (PO[3, mine] + R1[ab, rows].astype(F32)).astype(BF16)
                send(("second", part), S.at[2, ab, rows], R2.at[slot, ab, rows], large_axis(ab, step))

    second(0)
    second(1)
    arrived("direct", R1)

    def total_of(ab, rows):
        mine = slice(128 * ab + rows.start, 128 * ab + rows.stop)
        total = PO[0, mine] + R2[0, ab, rows].astype(F32)
        return mine, total + R2[1, ab, rows].astype(F32)

    arrived(("second", 0), R1.at[:, 0:32])
    for ab in range(2):
        for rows, to, step in ((slice(48, 64), slice(0, 16), 1), (slice(64, 80), slice(16, 32), 3)):
            TB[ab, rows] = total_of(ab, rows)[1].astype(BF16)
            send("first_small", TB.at[ab, rows], T1.at[ab, to], small_axis(ab, step))
    second(2)
    arrived(("second", 1), R1.at[:, 0:64])
    for ab in range(2):
        for rows, to, slot, step in (
            (slice(32, 48), slice(16, 32), 0, 1),
            (slice(80, 96), slice(0, 16), 1, 3),
        ):
            TB[ab, rows] = total_of(ab, rows)[1].astype(BF16)
            send("direct_small", TB.at[ab, rows], T2.at[slot, ab, to], small_axis(ab, step))
        for rows in (slice(16, 32), slice(96, 112)):
            mine, total = total_of(ab, rows)
            PO[0, mine] = total
    arrived("first_small", T1)
    for q, lanes in halves:
        for ab in range(2):
            for rows, half, slot, step in (
                (slice(16, 32), slice(0, 16), 0, 1),
                (slice(96, 112), slice(16, 32), 1, 3),
            ):
                mine = slice(128 * ab + rows.start, 128 * ab + rows.stop)
                TB[ab, rows, lanes] = (PO[0, mine, lanes] + T1[ab, half, lanes].astype(F32)).astype(BF16)
                send(("sent_small", q), TB.at[ab, rows, lanes], T2.at[slot, ab, half, lanes], small_axis(ab, step))
    arrived(("second", 2), R1.at[:, 0:32])
    for ab in range(2):
        for rows in (slice(0, 16), slice(112, 128)):
            mine, total = total_of(ab, rows)
            PO[0, mine] = total
    arrived("direct_small", T1)
    token_sums = []

    def small_total(q, lanes):
        arrived(("sent_small", q), T1.at[:, :, lanes])
        for ab in range(2):
            for top, half, first_z in ((0, slice(0, 16), 4 * ab), (112, slice(16, 32), 4 * ab + 2)):
                total = PO[0, 128 * ab + top : 128 * ab + top + 16, lanes]
                total += T2[0, ab, half, lanes].astype(F32)
                total += T2[1, ab, half, lanes].astype(F32)
                RET[first_z : first_z + 2, :, lanes] = total.reshape(2, CAP, FQ).astype(BF16)
        BACK[0, :, lanes] = RET[0, :, lanes]
        for j in (4, 3, 5, 2, 6, 1, 7):
            send(("back", q), RET.at[j, :, lanes], BACK.at[8 - j, :, lanes], at(dz=j))

    def mix(q, lanes):
        arrived(("back", q), BACK.at[1:8, :, lanes])
        back = BACK[:, :, lanes].astype(F32).reshape(NE * CAP, FQ).astype(BF16)
        three = jnp.dot(parts, back, preferred_element_type=F32)
        mixed = (three[0:16] + (three[16:32] + three[32:48])).astype(BF16)
        mixed_out[:, lanes] = mixed
        diff = mixed.astype(F32) - target[:, lanes].astype(F32)
        token_sums.append(jnp.sum(diff * diff, axis=1, keepdims=True))

    wavefront((small_total, mix), (0, 2))
    token_sum = sum(token_sums[1:], token_sums[0])
    sums = jnp.sum(bench_of * (token_sum / D), axis=0, keepdims=True)

    mine = z * 2 + c
    L1[mine] = sums
    for dz, dc in column:
        send("column", L1.at[mine], L1.at[mine], at(dz=dz, dc=dc))
    arrived("column", L1.at[0:15])
    mine = y * 4 + x
    L2[mine] = jnp.sum(L1[...], axis=0)
    for dy, dx in plane:
        send("plane", L2.at[mine], L2.at[mine], at(dy=dy, dx=dx))
    arrived("plane", L2.at[0:15])
    loss_sum = jnp.sum(L2[...], axis=0)
    loss_out[...] = (loss_sum / jnp.maximum(counts, 1.0))[:, 0:NB]
    counts_out[...] = counts[:, 0:NB].astype(jnp.int32)
    for copy in waits:
        copy.wait_send()


def hand_over(*refs):
    sources, targets, sems = refs[0:3], refs[3:6], refs[6]
    copies = [pltpu.make_async_copy(sources[i], targets[i], sems.at[i]) for i in range(3)]
    for copy in copies:
        copy.start()
    for copy in copies:
        copy.wait()


def per_device(tokens, target, router, w_gate, w_up, w_down, expert_ids, lengths, bench_ids):
    vmem = pl.BlockSpec(memory_space=pltpu.VMEM)
    hbm = pl.BlockSpec(memory_space=pltpu.HBM)
    mixed, loss, counts = pl.pallas_call(
        kernel,
        name="moe",
        out_shape=(
            pltpu.VMEM((TOK, DH), BF16),
            pltpu.VMEM((1, NB), F32),
            pltpu.VMEM((1, NB), jnp.int32),
        ),
        in_specs=[hbm] * 9,
        out_specs=(vmem, vmem, vmem),
        scratch_shapes=[
            pltpu.VMEM((TOK, DH), BF16),
            pltpu.VMEM((TOK, DH), BF16),
            pltpu.VMEM((NE, DH), BF16),
            pltpu.VMEM((2, TOK), jnp.int32),
            pltpu.VMEM((1, NSEQ), jnp.int32),
            pltpu.VMEM((1, NSEQ), jnp.int32),
            pltpu.VMEM((NE, CAP, DH), BF16),
            pltpu.VMEM((NE, CAP, DH), BF16),
            pltpu.VMEM((2, 32, DH), BF16),
            pltpu.VMEM((4, 2, 128, DH), BF16),
            pltpu.VMEM((4, 2, 128, DH), BF16),
            pltpu.VMEM((2, HID, DH), BF16),
            pltpu.VMEM((2, HID, DH), BF16),
            pltpu.VMEM((2, HID, DH), BF16),
            pltpu.VMEM((2, HID, 256), F32),
            pltpu.VMEM((256, HID), BF16),
            pltpu.VMEM((4, 256, DH), BF16),
            pltpu.VMEM((4, 256, DH), BF16),
            pltpu.VMEM((4, 256, DH), F32),
            pltpu.VMEM((3, 2, 128, DH), BF16),
            pltpu.VMEM((2, 128, DH), BF16),
            pltpu.VMEM((2, 2, 128, DH), BF16),
            pltpu.VMEM((2, 128, DH), BF16),
            pltpu.VMEM((2, 32, DH), BF16),
            pltpu.VMEM((2, 2, 32, DH), BF16),
            pltpu.VMEM((NE, CAP, DH), BF16),
            pltpu.VMEM((NE, CAP, DH), BF16),
            pltpu.VMEM((TOK, 128), F32),
            pltpu.VMEM((TOK, 128), F32),
            pltpu.VMEM((16, 1, 128), F32),
            pltpu.VMEM((16, 1, 128), F32),
            pltpu.SemaphoreType.DMA((12,)),
            pltpu.SemaphoreType.DMA((NSEMS,)),
            pltpu.SemaphoreType.DMA((NSEMS,)),
        ],
        compiler_params=pltpu.CompilerParams(
            collective_id=0, has_side_effects=True, vmem_limit_bytes=66 * 1000 * 1000
        ),
    )(
        tokens, target, router.T, w_gate.swapaxes(1, 2), w_up.swapaxes(1, 2), w_down, expert_ids.T,
        lengths.reshape(1, NSEQ), bench_ids.reshape(1, NSEQ),
    )
    mixed, loss, counts = pl.pallas_call(
        hand_over,
        name="hand_over",
        out_shape=(
            jax.ShapeDtypeStruct((TOK, DH), BF16),
            jax.ShapeDtypeStruct((1, NB), F32),
            jax.ShapeDtypeStruct((1, NB), jnp.int32),
        ),
        in_specs=[vmem, vmem, vmem],
        out_specs=(hbm, hbm, hbm),
        scratch_shapes=[pltpu.SemaphoreType.DMA((3,))],
        compiler_params=pltpu.CompilerParams(vmem_limit_bytes=4 * 1024 * 1024),
    )(mixed, loss, counts)
    return (mixed, loss.reshape(NB), counts.reshape(NB))


def solution(mesh):
    split = Mesh(
        mesh.devices.reshape(4, 4, mesh.shape["expert"], mesh.shape["tensor"]),
        ("dp_0", "dp_1", "expert", "tensor"),
    )
    in_specs = (
        P(DP_EXPERT, "tensor"),
        P(DP_EXPERT, "tensor"),
        P("tensor", None),
        P("expert", None, DP_TENSOR),
        P("expert", None, DP_TENSOR),
        P("expert", DP_TENSOR, None),
        P(DP_EXPERT, None),
        P(),
        P(),
    )
    out_specs = (P(DP_EXPERT, "tensor"), P(), P())
    return jax.shard_map(
        per_device, mesh=split, in_specs=in_specs, out_specs=out_specs, check_vma=False
    )
```

```python
import jax
import jax.numpy as jnp
from jax import lax
from jax.experimental import pallas as pl
from jax.experimental.pallas import tpu as pltpu
from jax.sharding import Mesh
from jax.sharding import PartitionSpec as P

D = 4096
DH = D // 2
NB = 16
CAP = 8
TOK = 16
HID = 448
NSEQ = 64
NE = 8
NQ = 2
FQ = DH // NQ
DP_EXPERT = ("dp_0", "dp_1", "expert")
DP_TENSOR = ("dp_0", "dp_1", "tensor")
MESH = pl.DeviceIdType.MESH
F32 = jnp.float32
BF16 = jnp.bfloat16
NSEMS = 48


def kernel(
    tokens_hbm, target_hbm, router_hbm, wg_hbm, wu_hbm, wd_hbm, ids_hbm, lengths_hbm, bench_hbm,
    mixed_out, loss_out, counts_out,
    tokens, target, router, ids, lengths, bench,
    OUT, ZL, ZR, XO, XP, WG, WU, WD, G, H, PX, PR, PO, S, R1, R2, TB, T1, T2, RET, BACK,
    LG, LGR, L1, L2, wsem, ssem, rsem,
):
    y = lax.axis_index("dp_0")
    x = lax.axis_index("dp_1")
    z = lax.axis_index("expert")
    c = lax.axis_index("tensor")

    def at(dy=0, dx=0, dz=0, dc=0):
        return {
            "dp_0": lax.rem(y + dy, 4),
            "dp_1": lax.rem(x + dx, 4),
            "expert": lax.rem(z + dz, 8),
            "tensor": lax.rem(c + dc, 2),
        }

    column = [(dz, dc) for dz in range(8) for dc in range(2)][1:]
    plane = [(dy, dx) for dy in range(4) for dx in range(4)][1:]
    barrier = pltpu.get_barrier_semaphore()
    for dz, dc in column:
        pl.semaphore_signal(barrier, inc=1, device_id=at(dz=dz, dc=dc), device_id_type=MESH)
    for dy, dx in plane:
        pl.semaphore_signal(barrier, inc=1, device_id=at(dy=dy, dx=dx), device_id_type=MESH)

    inputs = (
        (ids_hbm, ids), (tokens_hbm, tokens), (router_hbm, router),
        (target_hbm, target), (lengths_hbm, lengths), (bench_hbm, bench),
    )
    inputs = [pltpu.make_async_copy(src, dst, wsem.at[6 + i]) for i, (src, dst) in enumerate(inputs)]
    for copy in inputs:
        copy.start()
    loads = []
    for half in range(2):
        first = pl.multiple_of(lax.rem(c + half, 2) * DH, DH)
        loads.append(pltpu.make_async_copy(wg_hbm.at[0, :, pl.ds(first, DH)], WG.at[half], wsem.at[3 * half]))
        loads.append(pltpu.make_async_copy(wu_hbm.at[0, :, pl.ds(first, DH)], WU.at[half], wsem.at[3 * half + 1]))
        loads.append(pltpu.make_async_copy(wd_hbm.at[0, :, pl.ds(first, DH)], WD.at[half], wsem.at[3 * half + 2]))
    for load in loads:
        load.start()

    waits, numbers = [], {}

    def send(group, src, dst, device):
        number = numbers.setdefault(group, len(numbers))
        pltpu.make_async_remote_copy(
            src_ref=src, dst_ref=dst, send_sem=ssem.at[number], recv_sem=rsem.at[number],
            device_id=device, device_id_type=MESH,
        ).start()

    def arrived(group, region):
        number = numbers[group]
        copies = pltpu.make_async_remote_copy(
            src_ref=region, dst_ref=region, send_sem=ssem.at[number], recv_sem=rsem.at[number],
            device_id=at(dc=1), device_id_type=MESH,
        )
        copies.wait_recv()
        waits.append(copies)

    for copy in inputs:
        copy.wait()
    lane = lax.broadcasted_iota(jnp.int32, (TOK, 128), 1)
    row16 = lax.broadcasted_iota(jnp.int32, (TOK, TOK), 0)
    col16 = lax.broadcasted_iota(jnp.int32, (TOK, TOK), 1)

    def as_column(row):
        spread = jnp.broadcast_to(row.astype(F32), (TOK, TOK))
        return jnp.sum(jnp.where(row16 == col16, spread, 0.0), axis=1, keepdims=True).astype(jnp.int32)

    id_0 = as_column(ids[0:1, :])
    id_1 = as_column(ids[1:2, :])
    marks_0 = jnp.where(lane == id_0, 1.0, 0.0)
    marks_1 = jnp.where(lane == id_1, 1.0, 0.0)
    earlier = jnp.where(col16 < row16, 1.0, 0.0).astype(BF16)
    before = jnp.dot(earlier, (marks_0 + marks_1).astype(BF16), preferred_element_type=F32)
    slot_0 = jnp.sum(before * marks_0, axis=1, keepdims=True)
    slot_1 = jnp.sum(before * marks_1, axis=1, keepdims=True)
    place_0 = (((id_0 - z + NE) & (NE - 1)) * CAP).astype(F32) + slot_0
    place_1 = (((id_1 - z + NE) & (NE - 1)) * CAP).astype(F32) + slot_1
    place = lax.broadcasted_iota(jnp.int32, (TOK, NE * CAP), 1).astype(F32)
    put_0 = jnp.where(place == place_0, 1.0, 0.0)
    put_1 = jnp.where(place == place_1, 1.0, 0.0)
    dispatch = (put_0 + put_1).astype(BF16)
    for q in range(NQ):
        lanes = pl.ds(q * FQ, FQ)
        rows = lax.dot_general(
            dispatch, tokens[:, lanes], (((0,), (0,)), ((), ())), preferred_element_type=F32
        )
        rows = rows.reshape(NE, CAP, FQ).astype(BF16)
        OUT[:, :, lanes] = rows
        ZL[0, :, lanes] = rows[0]
    by_rows = (((1,), (1,)), ((), ()))
    partial = lax.dot_general(tokens[...], router[...], by_rows, preferred_element_type=F32)
    LG[...] = jnp.zeros((TOK, 128), F32)
    LG[:, 0:NE] = partial

    pl.semaphore_wait(barrier, len(column) + len(plane))

    for q in range(NQ):
        lanes = pl.ds(q * FQ, FQ)
        for j in (4, 3, 5, 2, 6, 1, 7):
            send(("z", q), OUT.at[j, :, lanes], ZL.at[8 - j, :, lanes], at(dz=j))
    send("logits", LG, LGR, at(dc=1))

    def small_axis(ab, step):
        return at(dx=step) if ab == 0 else at(dy=step)

    def large_axis(ab, step):
        return at(dy=step) if ab == 0 else at(dx=step)

    def wavefront(stages, lags):
        for tick in range(NQ + lags[-1]):
            for stage, lag in zip(stages, lags):
                if 0 <= tick - lag < NQ:
                    stage(tick - lag, pl.ds((tick - lag) * FQ, FQ))

    def from_z(q, lanes):
        arrived(("z", q), ZL.at[1:8, :, lanes])
        for ab in range(2):
            rows = ZL[4 * ab : 4 * ab + 4, :, lanes].astype(F32).reshape(32, FQ).astype(BF16)
            ZR[ab, :, lanes] = rows
            XO[0, ab, 0:16, lanes] = rows[0:16]
            XO[0, ab, 112:128, lanes] = rows[16:32]
        for ab in range(2):
            src = ZR.at[ab, :, lanes]
            send(("near_small", q, ab), src, XO.at[0, ab, 80:112, lanes], small_axis(ab, 1))
            send(("near_small", q, ab), src, XO.at[0, ab, 16:48, lanes], small_axis(ab, 3))
        for ab in range(2):
            early(q, lanes, ab, 0, 16)

    def early(q, lanes, ab, start, stop):
        for rows, step in ((slice(start, stop), 1), (slice(128 - stop, 128 - start), 3)):
            send(("near", q), XO.at[0, ab, rows, lanes], XO.at[1, ab, rows, lanes], large_axis(ab, step))

    def small_forward(q, lanes):
        for ab in range(2):
            arrived(("near_small", q, ab), XO.at[0, ab, 0:64, lanes])
            send(
                ("far_small", q, ab), XO.at[0, ab, 80:96, lanes], XO.at[0, ab, 48:64, lanes], small_axis(ab, 1)
            )
            send(
                ("far_small", q, ab), XO.at[0, ab, 32:48, lanes], XO.at[0, ab, 64:80, lanes], small_axis(ab, 3)
            )
        for ab in range(2):
            early(q, lanes, ab, 16, 48)

    def to_partner(unit, q, lanes):
        send(("across", unit, q), XO.at[unit, :, :, lanes], XP.at[unit, :, :, lanes], at(dc=1))

    def large_own(q, lanes):
        for ab in range(2):
            arrived(("far_small", q, ab), XO.at[0, ab, 0:32, lanes])
            early(q, lanes, ab, 48, 64)
        to_partner(0, q, lanes)
        if q == 0:
            late(0, lanes, 0, 32)

    def large_forward(q, lanes):
        arrived(("near", q), XO.at[1, :, :, lanes])
        for ab in range(2):
            send(("far", q), XO.at[1, ab, 0:64, lanes], XO.at[2, ab, 0:64, lanes], large_axis(ab, 1))
            send(("far", q), XO.at[1, ab, 64:128, lanes], XO.at[2, ab, 64:128, lanes], large_axis(ab, 3))
        to_partner(1, q, lanes)

    def late(q, lanes, lower, upper):
        for ab in range(2):
            for rows, step in ((slice(128 - upper, 128 - lower), 1), (slice(lower, upper), 3)):
                send(("late", q), XO.at[0, ab, rows, lanes], XO.at[3, ab, rows, lanes], large_axis(ab, step))

    wavefront((from_z, small_forward, large_own), (0, 1, 2))
    halves = [(q, pl.ds(q * FQ, FQ)) for q in range(NQ)]

    def up_own(unit):
        own = XO[unit].reshape(256, DH)
        G[0] = lax.dot_general(WG[0], own, by_rows, preferred_element_type=F32)
        G[1] = lax.dot_general(WU[0], own, by_rows, preferred_element_type=F32)

    def up_other(unit):
        for q, lanes in halves:
            arrived(("across", unit, q), XP.at[unit, :, :, lanes])
        other = XP[unit].reshape(256, DH)
        gate = G[0] + lax.dot_general(WG[1], other, by_rows, preferred_element_type=F32)
        raise_ = G[1] + lax.dot_general(WU[1], other, by_rows, preferred_element_type=F32)
        H[...] = (gate * jax.nn.sigmoid(gate) * raise_).astype(BF16).T

    def down(unit, between=None):
        for q, lanes in halves:
            for n in range(q * FQ, q * FQ + FQ, 512):
                cols = slice(n, n + 512)
                PX[unit, :, cols] = jnp.dot(H[...], WD[1, :, cols], preferred_element_type=F32).astype(BF16)
            send(("sums", unit, q), PX.at[unit, :, lanes], PR.at[unit, :, lanes], at(dc=1))
        if between is not None:
            between()
        for n in range(0, DH, 512):
            cols = slice(n, n + 512)
            PO[unit, :, cols] = jnp.dot(H[...], WD[0, :, cols], preferred_element_type=F32)

    def chip_sum(unit, q, lanes):
        arrived(("sums", unit, q), PR.at[unit, :, lanes])
        return PO[unit, :, lanes] + PR[unit, :, lanes].astype(F32)

    for load in loads:
        load.wait()
    up_own(0)
    arrived("logits", LGR)
    logits = LG[...] + LGR[...]
    picked_0 = jnp.sum(logits * marks_0, axis=1, keepdims=True)
    picked_1 = jnp.sum(logits * marks_1, axis=1, keepdims=True)
    gate_0 = jax.nn.sigmoid(picked_0 - picked_1)
    gate_1 = jax.nn.sigmoid(picked_1 - picked_0)
    weights = gate_0 * put_0 + gate_1 * put_1
    high = weights.astype(BF16)
    rest = weights - high.astype(F32)
    middle = rest.astype(BF16)
    low = (rest - middle.astype(F32)).astype(BF16)
    parts = jnp.concatenate([high, middle, low], axis=0)

    counted = lengths[...].astype(F32)
    row64 = lax.broadcasted_iota(jnp.int32, (NSEQ, NSEQ), 0)
    col64 = lax.broadcasted_iota(jnp.int32, (NSEQ, NSEQ), 1)
    upto = jnp.where(row64 <= col64, 1.0, 0.0).astype(BF16)
    wide = jnp.broadcast_to(counted, (8, NSEQ)).astype(BF16)
    ends = jnp.dot(wide, upto, preferred_element_type=F32)[0:1]
    starts = ends - counted
    first_token = ((y * 4 + x) * 8 + z) * TOK
    position = (first_token + lax.broadcasted_iota(jnp.int32, (TOK, NSEQ), 0)).astype(F32)
    inside = jnp.where((position >= starts) & (position < ends), 1.0, 0.0).astype(BF16)
    closing = jnp.max(jnp.where(position + 1.0 == ends, 1.0, 0.0), axis=1, keepdims=True)
    bench_row = lax.broadcasted_iota(jnp.int32, (128, NSEQ), 0)
    table = jnp.where(bench_row == bench[...], 1.0, 0.0).astype(BF16)
    bench_of = lax.dot_general(inside, table, by_rows, preferred_element_type=F32)
    bench_of = bench_of * (1.0 - closing)
    less_one = jnp.broadcast_to(counted - 1.0, (8, NSEQ)).astype(BF16)
    counts = lax.dot_general(less_one, table, by_rows, preferred_element_type=F32)[0:1]

    large_forward(*halves[0])
    up_other(0)
    large_forward(*halves[1])
    late(*halves[0], 32, 64)
    late(*halves[1], 0, 64)
    down(0)
    up_own(1)
    up_other(1)
    down(1)
    for q, lanes in halves:
        arrived(("far", q), XO.at[2, :, :, lanes])
        to_partner(2, q, lanes)
    up_own(2)
    for q, lanes in halves:
        S[0, :, :, lanes] = chip_sum(1, q, lanes).astype(BF16).reshape(2, 128, FQ)
    for ab in range(2):
        send("direct", S.at[0, ab, 64:128], R2.at[0, ab, 64:128], large_axis(ab, 1))
        send("direct", S.at[0, ab, 0:64], R2.at[1, ab, 0:64], large_axis(ab, 3))
    up_other(2)
    def last_block():
        for q, lanes in halves:
            arrived(("late", q), XO.at[3, :, :, lanes])
            to_partner(3, q, lanes)

    down(2, last_block)
    up_own(3)
    parts_of = ((48, 64), (16, 48), (0, 16))
    for q, lanes in halves:
        S[1, :, :, lanes] = chip_sum(2, q, lanes).astype(BF16).reshape(2, 128, FQ)
    for part, (start, stop) in enumerate(parts_of):
        for ab in range(2):
            for rows, step in ((slice(start, stop), 1), (slice(128 - stop, 128 - start), 3)):
                send(("first", part), S.at[1, ab, rows], R1.at[ab, rows], large_axis(ab, step))
    up_other(3)
    down(3)
    for q, lanes in halves:
        PO[0, :, lanes] = chip_sum(0, q, lanes)
    for q, lanes in halves:
        PO[3, :, lanes] = chip_sum(3, q, lanes)
    def second(part):
        start, stop = parts_of[part]
        arrived(("first", part), R1.at[:, 0 : 2 * (stop - start)])
        for ab in range(2):
            for slot, rows, step in ((0, slice(start, stop), 1), (1, slice(128 - stop, 128 - start), 3)):
                mine = slice(128 * ab + rows.start, 128 * ab + rows.stop)
                S[2, ab, rows] = (PO[3, mine] + R1[ab, rows].astype(F32)).astype(BF16)
                send(("second", part), S.at[2, ab, rows], R2.at[slot, ab, rows], large_axis(ab, step))

    second(0)
    second(1)
    arrived("direct", R1)

    def total_of(ab, rows):
        mine = slice(128 * ab + rows.start, 128 * ab + rows.stop)
        total = PO[0, mine] + R2[0, ab, rows].astype(F32)
        return mine, total + R2[1, ab, rows].astype(F32)

    arrived(("second", 0), R1.at[:, 0:32])
    for ab in range(2):
        for rows, to, step in ((slice(48, 64), slice(0, 16), 1), (slice(64, 80), slice(16, 32), 3)):
            TB[ab, rows] = total_of(ab, rows)[1].astype(BF16)
            send("first_small", TB.at[ab, rows], T1.at[ab, to], small_axis(ab, step))
    second(2)
    arrived(("second", 1), R1.at[:, 0:64])
    for ab in range(2):
        for rows, to, slot, step in (
            (slice(32, 48), slice(16, 32), 0, 1),
            (slice(80, 96), slice(0, 16), 1, 3),
        ):
            TB[ab, rows] = total_of(ab, rows)[1].astype(BF16)
            send("direct_small", TB.at[ab, rows], T2.at[slot, ab, to], small_axis(ab, step))
        for rows in (slice(16, 32), slice(96, 112)):
            mine, total = total_of(ab, rows)
            PO[0, mine] = total
    arrived("first_small", T1)
    for q, lanes in halves:
        for ab in range(2):
            for rows, half, slot, step in (
                (slice(16, 32), slice(0, 16), 0, 1),
                (slice(96, 112), slice(16, 32), 1, 3),
            ):
                mine = slice(128 * ab + rows.start, 128 * ab + rows.stop)
                TB[ab, rows, lanes] = (PO[0, mine, lanes] + T1[ab, half, lanes].astype(F32)).astype(BF16)
                send(("sent_small", q), TB.at[ab, rows, lanes], T2.at[slot, ab, half, lanes], small_axis(ab, step))
    arrived(("second", 2), R1.at[:, 0:32])
    for ab in range(2):
        for rows in (slice(0, 16), slice(112, 128)):
            mine, total = total_of(ab, rows)
            PO[0, mine] = total
    arrived("direct_small", T1)
    token_sums = []

    def small_total(q, lanes):
        arrived(("sent_small", q), T1.at[:, :, lanes])
        for ab in range(2):
            for top, half, first_z in ((0, slice(0, 16), 4 * ab), (112, slice(16, 32), 4 * ab + 2)):
                total = PO[0, 128 * ab + top : 128 * ab + top + 16, lanes]
                total += T2[0, ab, half, lanes].astype(F32)
                total += T2[1, ab, half, lanes].astype(F32)
                RET[first_z : first_z + 2, :, lanes] = total.reshape(2, CAP, FQ).astype(BF16)
        BACK[0, :, lanes] = RET[0, :, lanes]
        for j in (4, 3, 5, 2, 6, 1, 7):
            send(("back", q), RET.at[j, :, lanes], BACK.at[8 - j, :, lanes], at(dz=j))

    def mix(q, lanes):
        arrived(("back", q), BACK.at[1:8, :, lanes])
        back = BACK[:, :, lanes].astype(F32).reshape(NE * CAP, FQ).astype(BF16)
        three = jnp.dot(parts, back, preferred_element_type=F32)
        mixed = (three[0:16] + (three[16:32] + three[32:48])).astype(BF16)
        mixed_out[:, lanes] = mixed
        diff = mixed.astype(F32) - target[:, lanes].astype(F32)
        token_sums.append(jnp.sum(diff * diff, axis=1, keepdims=True))

    wavefront((small_total, mix), (0, 2))
    token_sum = sum(token_sums[1:], token_sums[0])
    sums = jnp.sum(bench_of * (token_sum / D), axis=0, keepdims=True)

    mine = z * 2 + c
    L1[mine] = sums
    for dz, dc in column:
        send("column", L1.at[mine], L1.at[mine], at(dz=dz, dc=dc))
    arrived("column", L1.at[0:15])
    mine = y * 4 + x
    L2[mine] = jnp.sum(L1[...], axis=0)
    for dy, dx in plane:
        send("plane", L2.at[mine], L2.at[mine], at(dy=dy, dx=dx))
    arrived("plane", L2.at[0:15])
    loss_sum = jnp.sum(L2[...], axis=0)
    loss_out[...] = (loss_sum / jnp.maximum(counts, 1.0))[:, 0:NB]
    counts_out[...] = counts[:, 0:NB].astype(jnp.int32)
    for copy in waits:
        copy.wait_send()


def hand_over(*refs):
    sources, targets, sems = refs[0:3], refs[3:6], refs[6]
    copies = [pltpu.make_async_copy(sources[i], targets[i], sems.at[i]) for i in range(3)]
    for copy in copies:
        copy.start()
    for copy in copies:
        copy.wait()


def per_device(tokens, target, router, w_gate, w_up, w_down, expert_ids, lengths, bench_ids):
    vmem = pl.BlockSpec(memory_space=pltpu.VMEM)
    hbm = pl.BlockSpec(memory_space=pltpu.HBM)
    mixed, loss, counts = pl.pallas_call(
        kernel,
        name="moe",
        out_shape=(
            pltpu.VMEM((TOK, DH), BF16),
            pltpu.VMEM((1, NB), F32),
            pltpu.VMEM((1, NB), jnp.int32),
        ),
        in_specs=[hbm] * 9,
        out_specs=(vmem, vmem, vmem),
        scratch_shapes=[
            pltpu.VMEM((TOK, DH), BF16),
            pltpu.VMEM((TOK, DH), BF16),
            pltpu.VMEM((NE, DH), BF16),
            pltpu.VMEM((2, TOK), jnp.int32),
            pltpu.VMEM((1, NSEQ), jnp.int32),
            pltpu.VMEM((1, NSEQ), jnp.int32),
            pltpu.VMEM((NE, CAP, DH), BF16),
            pltpu.VMEM((NE, CAP, DH), BF16),
            pltpu.VMEM((2, 32, DH), BF16),
            pltpu.VMEM((4, 2, 128, DH), BF16),
            pltpu.VMEM((4, 2, 128, DH), BF16),
            pltpu.VMEM((2, HID, DH), BF16),
            pltpu.VMEM((2, HID, DH), BF16),
            pltpu.VMEM((2, HID, DH), BF16),
            pltpu.VMEM((2, HID, 256), F32),
            pltpu.VMEM((256, HID), BF16),
            pltpu.VMEM((4, 256, DH), BF16),
            pltpu.VMEM((4, 256, DH), BF16),
            pltpu.VMEM((4, 256, DH), F32),
            pltpu.VMEM((3, 2, 128, DH), BF16),
            pltpu.VMEM((2, 128, DH), BF16),
            pltpu.VMEM((2, 2, 128, DH), BF16),
            pltpu.VMEM((2, 128, DH), BF16),
            pltpu.VMEM((2, 32, DH), BF16),
            pltpu.VMEM((2, 2, 32, DH), BF16),
            pltpu.VMEM((NE, CAP, DH), BF16),
            pltpu.VMEM((NE, CAP, DH), BF16),
            pltpu.VMEM((TOK, 128), F32),
            pltpu.VMEM((TOK, 128), F32),
            pltpu.VMEM((16, 1, 128), F32),
            pltpu.VMEM((16, 1, 128), F32),
            pltpu.SemaphoreType.DMA((12,)),
            pltpu.SemaphoreType.DMA((NSEMS,)),
            pltpu.SemaphoreType.DMA((NSEMS,)),
        ],
        compiler_params=pltpu.CompilerParams(
            collective_id=0, has_side_effects=True, vmem_limit_bytes=66 * 1000 * 1000
        ),
    )(
        tokens, target, router.T, w_gate.swapaxes(1, 2), w_up.swapaxes(1, 2), w_down, expert_ids.T,
        lengths.reshape(1, NSEQ), bench_ids.reshape(1, NSEQ),
    )
    mixed, loss, counts = pl.pallas_call(
        hand_over,
        name="hand_over",
        out_shape=(
            jax.ShapeDtypeStruct((TOK, DH), BF16),
            jax.ShapeDtypeStruct((1, NB), F32),
            jax.ShapeDtypeStruct((1, NB), jnp.int32),
        ),
        in_specs=[vmem, vmem, vmem],
        out_specs=(hbm, hbm, hbm),
        scratch_shapes=[pltpu.SemaphoreType.DMA((3,))],
        compiler_params=pltpu.CompilerParams(vmem_limit_bytes=4 * 1024 * 1024),
    )(mixed, loss, counts)
    return (mixed, loss.reshape(NB), counts.reshape(NB))


def solution(mesh):
    split = Mesh(
        mesh.devices.reshape(4, 4, mesh.shape["expert"], mesh.shape["tensor"]),
        ("dp_0", "dp_1", "expert", "tensor"),
    )
    in_specs = (
        P(DP_EXPERT, "tensor"),
        P(DP_EXPERT, "tensor"),
        P("tensor", None),
        P("expert", None, DP_TENSOR),
        P("expert", None, DP_TENSOR),
        P("expert", DP_TENSOR, None),
        P(DP_EXPERT, None),
        P(),
        P(),
    )
    out_specs = (P(DP_EXPERT, "tensor"), P(), P())
    return jax.shard_map(
        per_device, mesh=split, in_specs=in_specs, out_specs=out_specs, check_vma=False
    )
```
